32 devices in a mesh: grp: 2 (over y), reg: 4 (over z), sub: 4 (over x, core).
Axes of the slice: x: 2, y: 2, z: 4, core: 2. Of those that a mesh axis runs over, the one named last changes fastest.
Arguments:
- column_state: float32 [2, 128, 8192], P('grp', None, ('reg', 'sub')), may hold values from -6 to 6
- neighbours: int32 [2, 3, 8192], P('grp', None, ('reg', 'sub')), may hold values from 0 to 1055, as said below
- mixing: float32 [2, 128, 128], P('grp'), may hold values from -0.109375 to 0.109375
- diffusivity: float32 [2, 128], P('grp'), may hold values from 0.03 to 0.3
- flux_map: float32 [4, 128], replicated, may hold values from -0.625 to 0.625
- force_map: float32 [128, 4], replicated, may hold values from -3 to 3
- return_map: float32 [3, 128], replicated, may hold values from -0.5 to 0.5
- sources: int32 [3, 8192], P(None, ('reg', 'sub')), may hold values from 0 to 2047
- remap_weights: float32 [3, 8192], P(None, ('reg', 'sub')), may hold values from 0.1 to 0.6
- wet: int32 [8192], P(('reg', 'sub')), may hold values 0 or 1
Outputs:
- new_state: float32 [2, 128, 8192], P('grp', None, ('reg', 'sub'))
- coupled_surface: float32 [3, 8192], P(None, ('reg', 'sub'))
The draws below stay inside these ranges and needn't reach their ends.
Inputs may be any that keep to these rules, and one draw needn't show every extreme that they name: A cell's neighbours lie within 2 rows and 2 columns of it in its extended patch. sources point into the ocean cell's own slab.
All inputs are finite; a program needn't handle non-finite values. No bound on the sum of `wet` on one device may be relied on, other than what follows from the above.
Results may differ from the reference program's by a relative error of at most 0.0001.
Values sent between devices are 32-bit elements; how exact they have to be, the bound alone decides.
No kernel may reach another device: no remote copies, remote signals or barrier semaphores. Data moves between devices by JAX's collectives and lax.ppermute only.
A program may use at most 64 MiB of HBM per device.

```python
import math
import jax
import jax.numpy as jnp
from jax import lax

LEV = 128
LA = 90
CELLS = 512
BS = 128
HALO = 2
STEPS = 4
LINKS = 3
NF = 4
NR = 3
CELLS_ALL = 8192
N_REG = 4
N_SUB = 4


def draw_neighbours(key, part):
    place = jnp.arange(CELLS_ALL, dtype=jnp.int32) % CELLS
    prow = place // BS
    pcol = place % BS
    key_row = jax.random.fold_in(key, 11)
    key_col = jax.random.fold_in(key, 23)
    drow = jax.random.randint(key_row, (2, LINKS, CELLS_ALL), -HALO, HALO + 1, dtype=jnp.int32)
    dcol = jax.random.randint(key_col, (2, LINKS, CELLS_ALL), -HALO, HALO + 1, dtype=jnp.int32)
    index = (prow[None, None, :] + HALO + drow) * (BS + 2 * HALO) + (pcol[None, None, :] + HALO + dcol)
    return index.astype(jnp.int32)


def with_ends(drawn, rng, least, largest):
    longest = drawn.shape.index(max(drawn.shape))
    spots = []
    for shift in (0, 1):
        where = [jax.random.randint(jax.random.fold_in(rng, axis), (), 0, length) for axis, length in enumerate(drawn.shape)]
        where[longest] = (where[longest] + shift) % drawn.shape[longest]
        spots.append(tuple(where))
    return drawn.at[spots[0]].set(least).at[spots[1]].set(largest)


def shard_levels(key, extent, pieces, least, largest):
    def one(position, shards_of):
        steps = jax.random.uniform(jax.random.fold_in(jax.random.fold_in(key, 6), position), (shards_of,), jnp.float32, least / len(pieces), largest / len(pieces))
        return jnp.repeat(jnp.exp(steps), extent[position] // shards_of).reshape((-1,) + (1,) * (len(extent) - position - 1))

    gain = one(*pieces[0])
    for cut in pieces[1:]:
        gain = gain * one(*cut)
    return gain


def noise(own_key, extent, deviation, reach, shards=(), held_as=jnp.bfloat16):
    factor_of = shard_levels(own_key, extent, shards, -0.22, 0.18) if shards else 1.0
    array = jax.random.normal(own_key, extent, jnp.float32) * deviation * factor_of
    return jnp.minimum(jnp.maximum(array, -reach), reach).astype(held_as)


def setup_inputs(seed: int = 0) -> dict:
    seeds = jax.random.split(jax.random.key(seed), 11)
    column_state = noise(seeds[0], (2, LEV, CELLS_ALL), 1.0, 6.0, ((0, 2), (2, 16)), jnp.float32)
    neighbours = draw_neighbours(jax.random.fold_in(seeds[10], 71), 0)
    mixing = noise(seeds[2], (2, LEV, LEV), (25 * LEV) ** -0.5, 0.109375, ((0, 2),), jnp.float32)
    diffusivity = jnp.clip(jnp.exp(math.log(0.3) - 2.3025852 * jax.random.uniform(seeds[3], (2, LEV), jnp.float32) ** shard_levels(seeds[3], (2, LEV), ((0, 2),), -0.2, 0.2)), 0.03, 0.3)
    flux_map = noise(seeds[4], (NF, LEV), LA ** -0.5, 0.625, (), jnp.float32)
    force_map = noise(seeds[5], (LEV, NF), NF ** -0.5, 3.0, (), jnp.float32)
    return_map = noise(seeds[6], (NR, LEV), LEV ** -0.5, 0.5, (), jnp.float32)
    sources = with_ends(jax.random.randint(seeds[7], (LINKS, CELLS_ALL), 0, N_SUB * CELLS), jax.random.fold_in(seeds[7], 1), 0, (N_SUB * CELLS) - 1).astype(jnp.int32)
    remap_weights = jnp.clip(0.1 + 0.5 * jax.random.uniform(seeds[8], (LINKS, CELLS_ALL), jnp.float32) ** shard_levels(seeds[8], (LINKS, CELLS_ALL), ((1, 16),), -0.2, 0.2), 0.1, 0.6)
    wet = with_ends((jax.random.randint(seeds[9], (CELLS_ALL,), 0, 3) < 2).astype(jnp.int32), jax.random.fold_in(seeds[9], 1), 0, 1)
    return {"column_state": column_state, "neighbours": neighbours, "mixing": mixing, "diffusivity": diffusivity, "flux_map": flux_map, "force_map": force_map, "return_map": return_map, "sources": sources, "remap_weights": remap_weights, "wet": wet}


def extend(field):
    levels = field.shape[0]
    rows = CELLS // BS
    grid = field.reshape(levels, N_REG, N_SUB, rows, BS).transpose(0, 1, 3, 2, 4)
    grid = grid.reshape(levels, N_REG * rows, N_SUB * BS)
    return jnp.pad(grid, ((0, 0), (HALO, HALO), (HALO, HALO)), mode="wrap")


def spread(field, links, rate):
    rows = CELLS // BS
    padded = extend(field)
    cell = jnp.arange(CELLS_ALL, dtype=jnp.int32)
    slab = cell // (N_SUB * CELLS)
    block = (cell // CELLS) % N_SUB
    total = -float(LINKS) * field
    for k in range(LINKS):
        index = links[k].astype(jnp.int32)
        erow = index // (BS + 2 * HALO)
        ecol = index % (BS + 2 * HALO)
        taken = padded[:, slab * rows + erow, block * BS + ecol]
        total = total + taken
    return field + rate[:, None] * total


def mix(field, matrix):
    return field + jnp.dot(matrix, field, precision=lax.Precision.HIGHEST, preferred_element_type=jnp.float32)


def slab_targets(sources):
    cell = jnp.arange(CELLS_ALL, dtype=jnp.int32)
    base = (cell // (N_SUB * CELLS)) * (N_SUB * CELLS)
    return (base[None, :] + sources).astype(jnp.int32)


def reference(column_state, neighbours, mixing, diffusivity, flux_map, force_map, return_map, sources, remap_weights, wet):
    levels = jnp.arange(LEV, dtype=jnp.int32)[:, None]
    keep = (levels < LA).astype(jnp.float32)
    atmos = column_state[0] * keep
    flux = jnp.zeros((NF, CELLS_ALL), jnp.float32)
    for step in range(STEPS):
        atmos = keep * mix(spread(atmos, neighbours[0], diffusivity[0]), mixing[0])
        flux = flux + jnp.dot(flux_map, atmos, precision=lax.Precision.HIGHEST, preferred_element_type=jnp.float32)
    flux = flux / float(STEPS)
    targets = slab_targets(sources)
    ocean_flux = jnp.zeros((NF, CELLS_ALL), jnp.float32)
    for k in range(LINKS):
        ocean_flux = ocean_flux + remap_weights[k][None, :] * flux[:, targets[k]]
    wet_cells = wet.astype(jnp.float32)[None, :]
    start = column_state[1]
    pushed = spread(start, neighbours[1], diffusivity[1]) + jnp.dot(force_map, ocean_flux, precision=lax.Precision.HIGHEST, preferred_element_type=jnp.float32)
    ocean = start + wet_cells * (mix(pushed, mixing[1]) - start)
    new_state = jnp.stack([atmos, ocean], axis=0)
    surface = jnp.dot(return_map, ocean, precision=lax.Precision.HIGHEST, preferred_element_type=jnp.float32) * wet_cells
    coupled = jnp.zeros((NR, CELLS_ALL), jnp.float32)
    for k in range(LINKS):
        coupled = coupled.at[:, targets[k]].add(remap_weights[k][None, :] * surface)
    return new_state, coupled
```

```python
import functools
import jax
import jax.numpy as jnp
from jax import lax
from jax.experimental import pallas as pl
from jax.experimental.pallas import tpu as pltpu
from jax.sharding import PartitionSpec as P

LA = 90
BS = 128
HALO = 2
STEPS = 4
RIM = HALO * STEPS
TAPS = 2 * HALO + 1
HIGH = lax.Precision.HIGHEST
F32 = jnp.float32
BF16 = jnp.bfloat16
LANES = 128
WIDE = 2 * LANES


def up8(n):
    return -(-n // 8) * 8


def dot(a, b):
    return jnp.dot(a, b, precision=HIGH, preferred_element_type=F32)


def lane_of(width=LANES, rows=8):
    return lax.broadcasted_iota(jnp.int32, (rows, width), 1)


def roll(x, shift):
    shift = shift % x.shape[1]
    return x if shift == 0 else pltpu.roll(x, shift, 1)


def call(body, outs, *args, scratch=(), vmem=None, name=None, flops=100000):
    specs = [pl.BlockSpec(memory_space=pltpu.VMEM) for _ in args]
    size = sum(a.size * a.dtype.itemsize for a in args)
    return pl.pallas_call(
        body,
        out_shape=outs,
        in_specs=specs,
        out_specs=jax.tree.map(lambda _: pl.BlockSpec(memory_space=pltpu.VMEM), outs),
        scratch_shapes=list(scratch),
        compiler_params=pltpu.CompilerParams(vmem_limit_bytes=vmem),
        cost_estimate=pl.CostEstimate(flops=flops, bytes_accessed=size, transcendentals=0),
        name=name,
    )(*args)


def shape(*dims, dtype=F32):
    return jax.ShapeDtypeStruct(dims, dtype)


def pack_body(state, nbr, src, weight, wet, xin, up, dn, to_left, to_right, table):
    levels, cells = state.shape
    rows = cells // BS
    links = nbr.shape[0]
    ocean = lax.axis_index("grp") == 1
    sent = up.shape[0]
    half, edge = levels // 2, HALO * BS

    @pl.when(jnp.logical_not(ocean))
    def _():
        level = lax.broadcasted_iota(jnp.int32, (sent, cells), 0)
        xin[0:sent, :] = jnp.where(level < LA, state[0:sent, :], 0.0)
        xin[LA : LA + links, :] = nbr[...].astype(F32)
        if sent < levels:
            xin[sent:levels, :] = jnp.zeros((levels - sent, cells), F32)
        up[...] = xin[0:sent, :]
        dn[...] = xin[0:sent, :]

    @pl.when(ocean)
    def _():
        xin[...] = state[...]
        for part in range(2):
            rows_of = slice(part * half, (part + 1) * half)
            lanes_of = slice(part * edge, (part + 1) * edge)
            up[0:half, lanes_of] = state[rows_of, cells - edge : cells]
            dn[0:half, lanes_of] = state[rows_of, 0:edge]
        up[half:sent, :] = jnp.zeros((sent - half, cells), F32)
        dn[half:sent, :] = jnp.zeros((sent - half, cells), F32)

    lane = lane_of()
    quarter = levels // 4
    span = rows * RIM
    for g in range(quarter // 8):
        left = jnp.zeros((8, LANES), F32)
        right = jnp.zeros((8, LANES), F32)
        for q in range(4):
            for i in range(rows):
                at = q * span + i * RIM
                here = (lane >= at) & (lane < at + RIM)
                block = xin[q * quarter + 8 * g : q * quarter + 8 * g + 8, i * BS : (i + 1) * BS]
                left = jnp.where(here, roll(block, at), left)
                right = jnp.where(here, roll(block, at - (BS - RIM)), right)
        to_left[8 * g : 8 * g + 8, :] = left
        to_right[8 * g : 8 * g + 8, :] = right
    table[...] = jnp.zeros(table.shape, F32)
    table[0:links, :] = src[...].astype(F32)
    table[links : 2 * links, :] = weight[...]
    table[2 * links : 2 * links + 1, :] = wet[...].astype(F32)


def powers_body(mixing, rate, flux_map, fields, powers):
    levels = mixing.shape[0]
    nf = flux_map.shape[0]
    links = 3.0
    row = lax.broadcasted_iota(jnp.int32, (levels, levels), 0)
    col = lax.broadcasted_iota(jnp.int32, (levels, levels), 1)
    both = (row < LA) & (col < LA)
    base = jnp.where(both, mixing[...] + jnp.where(row == col, 1.0, 0.0), 0.0)
    r = rate[...]
    p0, p1 = base * (1.0 - links * r), base * r
    pair = jnp.concatenate([p0, p1], axis=1)

    lead = jnp.concatenate([flux_map[...], jnp.zeros((8 - nf, levels), F32)], axis=0)
    have = [lead]
    total = [jnp.zeros((8, levels), F32) for _ in range(STEPS + 1)]
    for n in range(1, STEPS + 1):
        out = dot(jnp.concatenate(have, axis=0) if len(have) > 1 else have[0], pair)
        new = []
        for j in range(n + 1):
            term = jnp.zeros((8, levels), F32)
            if j < n:
                term = term + out[8 * j : 8 * j + 8, :levels]
            if j > 0:
                term = term + out[8 * j - 8 : 8 * j, levels:]
            new.append(term)
            total[j] = total[j] + term
        have = new
    fields[...] = jnp.zeros(fields.shape, F32)
    for j in range(STEPS + 1):
        at = nf * ((j - 1) % (STEPS + 1))
        fields[at : at + nf, :] = total[j][0:nf, :] * (1.0 / STEPS)
    at = nf * (STEPS + 1)
    k = lax.broadcasted_iota(jnp.int32, (3, levels), 0)
    c = lax.broadcasted_iota(jnp.int32, (3, levels), 1)
    fields[at : at + 3, :] = jnp.where(c == LA + k, 1.0, 0.0)

    def squared(mats):
        n = len(mats)
        prod = dot(jnp.concatenate(mats, axis=0), jnp.concatenate(mats, axis=1))
        outs = []
        for j in range(2 * n - 1):
            term = None
            for a in range(n):
                b = j - a
                if 0 <= b < n:
                    piece = prod[a * levels : (a + 1) * levels, b * levels : (b + 1) * levels]
                    term = piece if term is None else term + piece
            outs.append(term)
        return outs

    mats = squared(squared([p0, p1]))
    keep = powers.shape[0]
    for j in range(STEPS + 1):
        powers[:, j * levels : (j + 1) * levels] = mats[j][0:keep, :]


def side_body(xin, from_right, from_left, fields, sides, ext, side_levels):
    levels, cells = xin.shape
    rows = cells // BS
    quarter, half = levels // 4, levels // 2
    span = rows * RIM
    lane = lane_of()
    for g in range(levels // 8):
        q, at = (8 * g) // quarter, (8 * g) % quarter
        a = roll(from_right[at : at + 8, :], -span * q)
        b = roll(from_left[at : at + 8, :], span - span * q)
        side_levels[8 * g : 8 * g + 8, :] = jnp.where(
            lane < span, a, jnp.where(lane < 2 * span, b, 0.0)
        )
    for g in range(half // 8):
        low = side_levels[8 * g : 8 * g + 8, :]
        high = side_levels[half + 8 * g : half + 8 * g + 8, :]
        sides[8 * g : 8 * g + 8, :] = low + roll(high, 2 * span)

    @pl.when(lax.axis_index("grp") == 0)
    def _():
        ext[:, 0:cells] = dot(fields[...], xin[...])
        ext[:, cells : cells + LANES] = dot(fields[...], side_levels[...])


def side_lanes(block, at_right, at_left):
    lane = lane_of()
    a = roll(block, -at_right)
    b = roll(block, LANES - RIM - at_left)
    return jnp.where(lane < RIM, a, jnp.where(lane >= LANES - RIM, b, 0.0))


def place_row(x_ref, i, at, blocks, side_of, rows):
    span = rows * RIM
    for g, (main, side, shift) in enumerate(blocks):
        x_ref[8 * g : 8 * g + 8, at * WIDE : at * WIDE + LANES] = main
        x_ref[8 * g : 8 * g + 8, at * WIDE + LANES : (at + 1) * WIDE] = side_lanes(
            side, shift + i * RIM, shift + span + i * RIM
        )


def tap_counts(codes, coef, rows, first_row, links):
    count, wide = codes.shape[1], codes.shape[2]
    row = (lax.broadcasted_iota(jnp.int32, (count, wide), 0) + first_row) % rows
    pcol = lax.broadcasted_iota(jnp.int32, (count, wide), 1) % LANES
    width = BS + 2 * HALO
    kinds = []
    for k in range(links):
        n = codes[k].astype(jnp.int32)
        line = ((n.astype(F32) + 0.5) * (1.0 / width)).astype(jnp.int32)
        kinds.append((line - row) * 16 + (n - line * width - pcol))
    for dr in range(TAPS):
        for dc in range(TAPS):
            hits = jnp.zeros((count, wide), F32)
            for k in range(links):
                hits = hits + jnp.where(kinds[k] == dr * 16 + dc, 1.0, 0.0)
            coef[dr * TAPS + dc] = roll(hits, dc - HALO)


def stencil(src, dst, coef, groups, first, count, batch):
    def one(i, _):
        off = [pl.multiple_of((i + dr - HALO) * WIDE, WIDE) for dr in range(TAPS)]
        here = pl.multiple_of(i * WIDE, WIDE)
        for g0 in range(0, groups, batch):
            gs = range(g0, min(g0 + batch, groups))
            acc = {}
            for dr in range(TAPS):
                v = {g: src[8 * g : 8 * g + 8, pl.ds(off[dr], WIDE)] for g in gs}
                for dc in range(TAPS):
                    c = coef[dr * TAPS + dc, pl.ds(i, 1), :]
                    for g in gs:
                        t = c * v[g]
                        acc[g, dc] = t if dr == 0 else acc[g, dc] + t
            for g in gs:
                total = acc[g, HALO]
                for dc in range(TAPS):
                    if dc != HALO:
                        total = total + roll(acc[g, dc], HALO - dc)
                dst[8 * g : 8 * g + 8, pl.ds(here, WIDE)] = total
        return 0

    lax.fori_loop(first, first + count, one, 0)


def chain(xa, xb, coef, groups, rows, near, batch, take):
    total = rows * (2 * near + 1)
    refs = (xa, xb)
    lo = near * rows
    take(0, xa, lo)
    for j in range(1, STEPS + 1):
        src, dst = refs[(j - 1) % 2], refs[j % 2]
        first = lo - RIM + HALO * j
        stencil(src, dst, coef, groups, first, total - 2 * first, batch)
        take(j, dst, lo)


def flux_body(rows, near, nf, links, *refs):
    n = 2 * near + 1
    blocks, (q8, out, xa, xb, codes, coef) = refs[:n], refs[n:]
    cells = rows * BS
    groups = nf * STEPS // 8
    nbr = nf * (STEPS + 1)

    @pl.when(lax.axis_index("grp") == 1)
    def _():
        total = rows * n
        codes[...] = jnp.zeros(codes.shape, F32)
        tail = 8 * (nbr // 8)
        for d in range(n):
            for i in range(rows):
                at = d * rows + i
                parts = [
                    (
                        blocks[d][8 * g : 8 * g + 8, i * BS : (i + 1) * BS],
                        blocks[d][8 * g : 8 * g + 8, cells : cells + LANES],
                        0,
                    )
                    for g in range(groups)
                ]
                place_row(xa, i, at, parts, None, rows)
                main = blocks[d][tail : tail + 8, i * BS : (i + 1) * BS]
                side = side_lanes(
                    blocks[d][tail : tail + 8, cells : cells + LANES], i * RIM, (rows + i) * RIM
                )
                for k in range(links):
                    s = nbr - tail + k
                    codes[k, at : at + 1, 0:LANES] = main[s : s + 1, :]
                    codes[k, at : at + 1, LANES:WIDE] = side[s : s + 1, :]
        tap_counts(codes, coef, rows, 0, links)
        own = blocks[near]
        out[0:nf, :] = own[nf * STEPS : nf * (STEPS + 1), 0:cells]
        out[nf:8, :] = q8[0 : 8 - nf, :]

        def take(j, ref, lo):
            if j == 0:
                return
            at = nf * (j - 1)
            for i in range(rows):
                here = slice(i * BS, (i + 1) * BS)
                out[0:nf, here] = (
                    out[0:nf, here] + ref[at : at + nf, (lo + i) * WIDE : (lo + i) * WIDE + LANES]
                )

        chain(xa, xb, coef, groups, rows, near, groups, take)


def ocean_body(rows, links, xin, nbr, above, below, sides, sides_above, sides_below,
               mixing, rate, force_map, return_map, mixed, q8, lift, x, y, codes, coef):
    levels, cells = xin.shape
    half, edge = levels // 2, HALO * BS
    groups = levels // 8
    nr, nf = return_map.shape[0], force_map.shape[1]

    @pl.when(lax.axis_index("grp") == 1)
    def _():
        for at in range(rows + 2 * HALO):
            if at < HALO:
                i, side = rows - HALO + at, sides_above
            elif at < HALO + rows:
                i, side = at - HALO, sides
            else:
                i, side = at - HALO - rows, sides_below
            parts = []
            for g in range(groups):
                part, gs = divmod(8 * g, half)
                if at < HALO:
                    main = above[gs : gs + 8, part * edge + at * BS : part * edge + (at + 1) * BS]
                elif at < HALO + rows:
                    main = xin[8 * g : 8 * g + 8, i * BS : (i + 1) * BS]
                else:
                    main = below[gs : gs + 8, part * edge + i * BS : part * edge + (i + 1) * BS]
                parts.append((main, side[gs : gs + 8, :], part * 2 * rows * RIM))
            place_row(x, i, at, parts, None, rows)
        codes[...] = jnp.zeros(codes.shape, F32)
        for k in range(links):
            for i in range(rows):
                codes[k, HALO + i : HALO + i + 1, 0:LANES] = nbr[
                    k : k + 1, i * BS : (i + 1) * BS
                ].astype(F32)
        tap_counts(codes, coef, rows, rows - HALO, links)
        stencil(x, y, coef, groups, HALO, rows, 3)
        matrix = mixing[...]
        r = rate[...]
        out = return_map[...]
        for i in range(rows):
            own = xin[:, i * BS : (i + 1) * BS]
            near = y[:, (HALO + i) * WIDE : (HALO + i) * WIDE + LANES]
            spread = own + r * (near - float(links) * own)
            now = spread + dot(matrix, spread)
            mixed[:, i * BS : (i + 1) * BS] = now
        q8[...] = jnp.zeros(q8.shape, F32)
        q8[0:nr, :] = dot(out, mixed[...])
        force = force_map[...]
        lifted = force + dot(matrix, force)
        lift[...] = jnp.zeros(lift.shape, F32)
        lift[0:levels, 0:nf] = lifted
        lift[levels : levels + nr, 0:nf] = dot(out, lifted)


def onto_body(links, count, *refs):
    tables, (high, low, whole) = refs[:count], refs[count:]
    cells = tables[0].shape[1]
    me = lax.axis_index("sub")
    for d in range(count):
        at = pl.multiple_of(((me + d) % count) * cells, cells)
        whole[:, pl.ds(at, cells)] = tables[d][...]

    @pl.when(lax.axis_index("grp") == 1)
    def _():
        def chunk(c, _):
            at = pl.multiple_of(c * LANES, LANES)
            src = whole[0:links, pl.ds(at, LANES)].astype(jnp.int32) - me * cells
            w = whole[links : 2 * links, pl.ds(at, LANES)]
            for t in range(0, cells, 16):
                target = lax.broadcasted_iota(jnp.int32, (16, LANES), 0) + t
                value = jnp.zeros((16, LANES), F32)
                for k in range(links):
                    value = value + jnp.where(src[k : k + 1, :] == target, w[k : k + 1, :], 0.0)
                top = value.astype(BF16)
                high[t : t + 16, pl.ds(at, LANES)] = top
                low[t : t + 16, pl.ds(at, LANES)] = (value - top.astype(F32)).astype(BF16)
            return 0

        lax.fori_loop(0, count * cells // LANES, chunk, 0)


def couple_body(links, nf, nr, count, *refs):
    blocks, (whole, high, low, lift, own_flux, out, slab, surface) = refs[:count], refs[count:]
    cells = blocks[0].shape[1]
    levels = lift.shape[0] - 8
    me = lax.axis_index("sub")
    for d in range(count):
        at = pl.multiple_of(((me + d) % count) * cells, cells)
        slab[:, pl.ds(at, cells)] = blocks[d][...]

    @pl.when(lax.axis_index("grp") == 1)
    def _():
        chunks = count * cells // LANES
        per = min(chunks, 16)

        def target(c, _):
            at = pl.multiple_of(c * LANES, LANES)
            table = whole[:, pl.ds(at, LANES)]
            src = table.astype(jnp.int32)
            lanes = [
                jnp.broadcast_to(src[k : k + 1, :] % LANES, (8, LANES)) for k in range(links)
            ]
            homes = [
                jnp.broadcast_to(src[k : k + 1, :] // LANES, (8, LANES)) for k in range(links)
            ]

            def source(o, acc):
                acc = list(acc)
                for p in range(per):
                    b = o * per + p
                    v = slab[:, pl.ds(pl.multiple_of(b * LANES, LANES), LANES)]
                    for k in range(links):
                        got = jnp.take_along_axis(v, lanes[k], axis=1)
                        acc[k] = jnp.where(homes[k] == b, got, acc[k])
                return tuple(acc)

            zero = tuple(jnp.zeros((8, LANES), F32) for _ in range(links))
            if chunks == per:
                got = source(0, zero)
            else:
                got = lax.fori_loop(0, chunks // per, source, zero)
            flux = jnp.zeros((8, LANES), F32)
            for k in range(links):
                flux = flux + table[links + k : links + k + 1, :] * got[k]
            own = slab[:, pl.ds(at, LANES)]
            face = own[nf : nf + nr, :]
            for f in range(nf):
                face = face + lift[levels : levels + nr, f : f + 1] * flux[f : f + 1, :]
            face = face * table[2 * links : 2 * links + 1, :]
            surface[0:nr, pl.ds(at, LANES)] = face
            surface[nr:8, pl.ds(at, LANES)] = jnp.zeros((8 - nr, LANES), F32)
            here = c - me * (cells // LANES)

            @pl.when((here >= 0) & (here < cells // LANES))
            def _():
                own_flux[:, pl.ds(pl.multiple_of(here * LANES, LANES), LANES)] = flux

            return 0

        lax.fori_loop(0, chunks, target, 0)
        face = surface[...]
        top = face.astype(BF16)
        rest = (face - top.astype(F32)).astype(BF16)
        both = jnp.concatenate([top, rest], axis=0)

        def nt(a, b):
            return lax.dot_general(
                a, b[...], (((1,), (1,)), ((), ())), preferred_element_type=F32
            )

        one = nt(both, high)
        two = nt(both, low)
        out[...] = one[0:8, :] + one[8:16, :] + two[0:8, :]


def state_body(rows, near, links, sent, *refs):
    n = 2 * near + 1
    mains, sides = refs[:n], refs[n : 2 * n]
    (powers, mixed, own_flux, lift, wet, out, xa, xb, codes, coef, basis) = refs[2 * n :]
    levels, cells = out.shape
    groups = sent // 8
    half = levels // 2
    ocean = lax.axis_index("grp") == 1

    @pl.when(ocean)
    def _():
        start = mains[near][...]
        now = mixed[...] + dot(lift[0:levels, 0:8], own_flux[...])
        out[...] = start + wet[...].astype(F32) * (now - start)

    @pl.when(jnp.logical_not(ocean))
    def _():
        codes[...] = jnp.zeros(codes.shape, F32)
        tail = 8 * (LA // 8)
        for d in range(n):
            for i in range(rows):
                at = d * rows + i
                parts = []
                for g in range(groups):
                    part, gs = divmod(8 * g, half)
                    parts.append(
                        (
                            mains[d][8 * g : 8 * g + 8, i * BS : (i + 1) * BS],
                            sides[d][gs : gs + 8, :],
                            part * 2 * rows * RIM,
                        )
                    )
                place_row(xa, i, at, parts, None, rows)
                for k in range(links):
                    s = LA + k
                    codes[k, at : at + 1, :] = xa[s : s + 1, at * WIDE : (at + 1) * WIDE]
        tap_counts(codes, coef, rows, 0, links)
        basis[...] = jnp.zeros(basis.shape, F32)

        def take(j, ref, lo):
            for i in range(rows):
                basis[j * levels : j * levels + sent, i * BS : (i + 1) * BS] = ref[
                    0:sent, (lo + i) * WIDE : (lo + i) * WIDE + LANES
                ]

        chain(xa, xb, coef, groups, rows, near, 3, take)
        out[0:sent, :] = dot(powers[...], basis[...])
        if sent < levels:
            out[sent:levels, :] = jnp.zeros((levels - sent, cells), F32)


def local(
    column_state,
    neighbours,
    mixing,
    diffusivity,
    flux_map,
    force_map,
    return_map,
    sources,
    remap_weights,
    wet,
):
    state = column_state[0]
    nbr = neighbours[0]
    levels, cells = state.shape
    rows = cells // BS
    links = nbr.shape[0]
    nf, nr = flux_map.shape[0], return_map.shape[0]
    near = -(-RIM // rows)
    n = 2 * near + 1
    sent = max(up8(LA + links), levels // 2)
    n_reg, n_sub = lax.axis_size("reg"), lax.axis_size("sub")
    axes = ("grp", "reg", "sub")
    wet_row = wet.reshape(1, cells)

    def at(g, r, s):
        return (g * n_reg + r % n_reg) * n_sub + s % n_sub

    spots = [(r, s) for r in range(n_reg) for s in range(n_sub)]

    def shift(x, axis, d):
        size = lax.axis_size(axis)
        return lax.ppermute(x, axis, [((i + d) % size, i) for i in range(size)])

    ext_rows = up8(nf * (STEPS + 1) + links)
    xin, up, dn, to_left, to_right, table = call(
        pack_body,
        (
            shape(levels, cells),
            shape(sent, cells),
            shape(sent, cells),
            shape(levels // 4, LANES),
            shape(levels // 4, LANES),
            shape(8, cells),
        ),
        state, nbr, sources, remap_weights, wet_row,
        name="pack", vmem=8 << 20,
    )
    from_right = shift(to_left, "sub", 1)
    from_left = shift(to_right, "sub", -1)
    rate_row = diffusivity
    fields, powers = call(
        powers_body,
        (shape(ext_rows, levels), shape(sent, (STEPS + 1) * levels)),
        mixing[0], rate_row, flux_map,
        name="powers", vmem=8 << 20,
    )
    sides, ext = call(
        side_body,
        (shape(levels // 2, LANES), shape(ext_rows, cells + LANES)),
        xin, from_right, from_left, fields,
        scratch=[pltpu.VMEM((levels, LANES), F32)],
        name="side", vmem=8 << 20,
    )

    got = {}
    for d in range(-near, near + 1):
        key = d % n_reg
        if key not in got:
            got[key] = lax.ppermute(ext, axes, [(at(0, r + d, s), at(1, r, s)) for r, s in spots])
    ext_blocks = [got[d % n_reg] for d in range(-near, near + 1)]

    mains, side_blocks = {0: xin}, {0: sides}
    for d in sorted(range(-near, near + 1), key=abs):
        if d % n_reg in mains:
            continue
        block = up if d < 0 else dn
        groups = (0, 1) if abs(d) == 1 else (0,)
        pairs = [(at(g, r + d, s), at(g, r, s)) for g in groups for r, s in spots]
        mains[d % n_reg] = lax.ppermute(block, axes, pairs)
        side_blocks[d % n_reg] = lax.ppermute(sides, axes, pairs)
    order = [d % n_reg for d in range(-near, near + 1)]

    tables = [table] + [shift(table, "sub", d) for d in range(1, n_sub)]
    span = n_sub * cells
    high, low, whole = call(
        functools.partial(onto_body, links, n_sub),
        (shape(cells, span, dtype=BF16), shape(cells, span, dtype=BF16), shape(8, span)),
        *tables,
        name="onto", vmem=24 << 20,
    )

    ext_o = up8(rows + 2 * HALO)
    mixed, q8, lift = call(
        functools.partial(ocean_body, rows, links),
        (shape(levels, cells), shape(8, cells), shape(levels + 8, LANES)),
        xin, nbr, mains[-1 % n_reg], mains[1 % n_reg], sides,
        side_blocks[-1 % n_reg], side_blocks[1 % n_reg],
        mixing[0], diffusivity.reshape(levels, 1), force_map, return_map,
        scratch=[
            pltpu.VMEM((levels, (rows + 2 * HALO) * WIDE), F32),
            pltpu.VMEM((levels, (rows + 2 * HALO) * WIDE), F32),
            pltpu.VMEM((links, ext_o, WIDE), F32),
            pltpu.VMEM((TAPS * TAPS, ext_o, WIDE), F32),
        ],
        name="ocean", vmem=16 << 20,
    )

    total = rows * n
    ext_n = up8(total)
    fq = call(
        functools.partial(flux_body, rows, near, nf, links),
        shape(8, cells),
        *ext_blocks, q8,
        scratch=[
            pltpu.VMEM((nf * STEPS, total * WIDE), F32),
            pltpu.VMEM((nf * STEPS, total * WIDE), F32),
            pltpu.VMEM((links, ext_n, WIDE), F32),
            pltpu.VMEM((TAPS * TAPS, ext_n, WIDE), F32),
        ],
        name="flux", vmem=8 << 20,
    )
    blocks = [fq] + [shift(fq, "sub", d) for d in range(1, n_sub)]
    own_flux, coupled = call(
        functools.partial(couple_body, links, nf, nr, n_sub),
        (shape(8, cells), shape(8, cells)),
        *blocks, whole, high, low, lift,
        scratch=[pltpu.VMEM((8, span), F32), pltpu.VMEM((8, span), F32)],
        name="couple", vmem=24 << 20,
    )
    back = lax.ppermute(coupled, axes, [(at(1, r, s), at(0, r, s)) for r, s in spots])

    new_state = call(
        functools.partial(state_body, rows, near, links, sent),
        shape(levels, cells),
        *[mains[d] for d in order], *[side_blocks[d] for d in order],
        powers, mixed, own_flux, lift, wet_row,
        scratch=[
            pltpu.VMEM((sent, total * WIDE), F32),
            pltpu.VMEM((sent, total * WIDE), F32),
            pltpu.VMEM((links, ext_n, WIDE), F32),
            pltpu.VMEM((TAPS * TAPS, ext_n, WIDE), F32),
            pltpu.VMEM(((STEPS + 1) * levels, cells), F32),
        ],
        name="state", vmem=24 << 20,
    )
    ocean_side = lax.axis_index("grp") == 1
    surface = jnp.where(ocean_side, coupled[:nr], back[:nr])
    return (new_state[None], surface)


def solution(mesh):
    in_specs = (
        P("grp", None, ("reg", "sub")),
        P("grp", None, ("reg", "sub")),
        P("grp", None, None),
        P("grp", None),
        P(),
        P(),
        P(),
        P(None, ("reg", "sub")),
        P(None, ("reg", "sub")),
        P(("reg", "sub")),
    )
    out_specs = (P("grp", None, ("reg", "sub")), P(None, ("reg", "sub")))
    return jax.shard_map(local, mesh=mesh, in_specs=in_specs, out_specs=out_specs, check_vma=False)
```

```python
import functools
import jax
import jax.numpy as jnp
from jax import lax
from jax.experimental import pallas as pl
from jax.experimental.pallas import tpu as pltpu
from jax.sharding import PartitionSpec as P

LA = 90
BS = 128
HALO = 2
STEPS = 4
RIM = HALO * STEPS
TAPS = 2 * HALO + 1
HIGH = lax.Precision.HIGHEST
F32 = jnp.float32
BF16 = jnp.bfloat16
LANES = 128
WIDE = 2 * LANES


def up8(n):
    return -(-n // 8) * 8


def dot(a, b):
    return jnp.dot(a, b, precision=HIGH, preferred_element_type=F32)


def lane_of(width=LANES, rows=8):
    return lax.broadcasted_iota(jnp.int32, (rows, width), 1)


def roll(x, shift):
    shift = shift % x.shape[1]
    return x if shift == 0 else pltpu.roll(x, shift, 1)


def call(body, outs, *args, scratch=(), vmem=None, flops=100000, space=pltpu.VMEM):
    size = sum(a.size * a.dtype.itemsize for a in args)
    return pl.pallas_call(
        body,
        out_shape=outs,
        in_specs=[pl.BlockSpec(memory_space=space) for _ in args],
        out_specs=jax.tree.map(lambda _: pl.BlockSpec(memory_space=pltpu.VMEM), outs),
        scratch_shapes=list(scratch),
        compiler_params=pltpu.CompilerParams(vmem_limit_bytes=vmem),
        cost_estimate=pl.CostEstimate(flops=flops, bytes_accessed=size, transcendentals=0),
    )(*args)


def shape(*dims, dtype=F32):
    return jax.ShapeDtypeStruct(dims, dtype)


def pack_body(links, state, cell_in, xin, to_left, to_right, table):
    levels, cells = xin.shape
    rows = cells // BS
    ocean = lax.axis_index("grp") == 1

    @pl.when(jnp.logical_not(ocean))
    def _():
        level = lax.broadcasted_iota(jnp.int32, (levels, cells), 0)
        xin[...] = jnp.where(level < LA, state[...], 0.0)
        xin[LA : LA + links, :] = cell_in[0:links, :]

    @pl.when(ocean)
    def _():
        xin[...] = state[...]

    lane = lane_of()
    quarter = levels // 4
    span = rows * RIM
    for g in range(quarter // 8):
        left = jnp.zeros((8, LANES), F32)
        right = jnp.zeros((8, LANES), F32)
        for q in range(4):
            for i in range(rows):
                at = q * span + i * RIM
                here = (lane >= at) & (lane < at + RIM)
                block = xin[q * quarter + 8 * g : q * quarter + 8 * g + 8, i * BS : (i + 1) * BS]
                left = jnp.where(here, roll(block, at), left)
                right = jnp.where(here, roll(block, at - (BS - RIM)), right)
        to_left[8 * g : 8 * g + 8, :] = left
        to_right[8 * g : 8 * g + 8, :] = right
    table[...] = cell_in[links : links + 8, :]
    for c in range(cells // LANES):
        part = table[:, c * LANES : (c + 1) * LANES]
        to_left[quarter + 8 * c : quarter + 8 * c + 8, :] = part
        to_right[quarter + 8 * c : quarter + 8 * c + 8, :] = part


def level_matrix(mixing):
    levels = mixing.shape[0]
    row = lax.broadcasted_iota(jnp.int32, (levels, levels), 0)
    col = lax.broadcasted_iota(jnp.int32, (levels, levels), 1)
    full = mixing[...] + jnp.where(row == col, 1.0, 0.0)
    return full, jnp.where((row < LA) & (col < LA), full, 0.0)


def fields_body(nf, nr, links, mixing, small, fields, face0):
    levels = mixing.shape[0]
    full, base = level_matrix(mixing)
    r = small[0:1, :]
    ocean = lax.axis_index("grp") == 1
    at = nf * STEPS
    fields[...] = jnp.zeros(fields.shape, F32)

    @pl.when(jnp.logical_not(ocean))
    def _():
        pair = jnp.concatenate([base * (1.0 - float(links) * r), base * r], axis=1)
        lead = jnp.concatenate([small[1 : 1 + nf, :], jnp.zeros((8 - nf, levels), F32)], axis=0)
        have = [lead]
        total = [jnp.zeros((8, levels), F32) for _ in range(STEPS + 1)]
        for n in range(1, STEPS + 1):
            out = dot(jnp.concatenate(have, axis=0) if len(have) > 1 else have[0], pair)
            new = []
            for j in range(n + 1):
                term = jnp.zeros((8, levels), F32)
                if j < n:
                    term = term + out[8 * j : 8 * j + 8, :levels]
                if j > 0:
                    term = term + out[8 * j - 8 : 8 * j, levels:]
                new.append(term)
                total[j] = total[j] + term
            have = new
        for j in range(STEPS + 1):
            to = nf * ((j - 1) % (STEPS + 1))
            fields[to : to + nf, :] = total[j][0:nf, :] * (1.0 / STEPS)
        k = lax.broadcasted_iota(jnp.int32, (links, levels), 0)
        c = lax.broadcasted_iota(jnp.int32, (links, levels), 1)
        fields[at + nf : at + nf + links, :] = jnp.where(c == LA + k, 1.0, 0.0)
        face0[...] = jnp.zeros(face0.shape, F32)

    @pl.when(ocean)
    def _():
        first = 1 + 2 * nf
        lead = jnp.concatenate(
            [small[first : first + nr, :], jnp.zeros((8 - nr, levels), F32)], axis=0
        )
        through = dot(lead, full)
        face0[...] = through * (1.0 - float(links) * r)
        fields[at : at + nr, :] = (through * r)[0:nr, :]


def powers_body(nf, nr, links, mixing, small, powers, own_mix, lift):
    levels = mixing.shape[0]
    full, base = level_matrix(mixing)
    r = small[0:1, :]
    ocean = lax.axis_index("grp") == 1

    @pl.when(jnp.logical_not(ocean))
    def _():
        def squared(mats):
            n = len(mats)
            prod = dot(jnp.concatenate(mats, axis=0), jnp.concatenate(mats, axis=1))
            outs = []
            for j in range(2 * n - 1):
                term = None
                for a in range(n):
                    b = j - a
                    if 0 <= b < n:
                        piece = prod[a * levels : (a + 1) * levels, b * levels : (b + 1) * levels]
                        term = piece if term is None else term + piece
                outs.append(term)
            return outs

        mats = squared(squared([base * (1.0 - float(links) * r), base * r]))
        keep = powers.shape[0]
        for j in range(STEPS + 1):
            powers[:, j * levels : (j + 1) * levels] = mats[j][0:keep, :]

    @pl.when(ocean)
    def _():
        own_mix[:, 0:levels] = full * (1.0 - float(links) * r)
        own_mix[:, levels : 2 * levels] = full * r
        first = 1 + 2 * nf
        lead = jnp.concatenate(
            [small[first : first + nr, :], jnp.zeros((8 - nr, levels), F32)], axis=0
        )
        top = jnp.concatenate(
            [small[1 + nf : 1 + 2 * nf, :], jnp.zeros((8 - nf, levels), F32)], axis=0
        )
        lifted = lax.dot_general(
            full, top, (((1,), (1,)), ((), ())), precision=HIGH, preferred_element_type=F32
        )
        lift[0:levels, :] = lifted
        lift[levels : levels + 8, :] = dot(lead, lifted)


def side_body(xin, from_right, from_left, fields, face0, up, dn, ext, q0, side_levels):
    levels, cells = xin.shape
    rows = cells // BS
    quarter, half = levels // 4, levels // 2
    span = rows * RIM
    lane = lane_of()
    ocean = lax.axis_index("grp") == 1
    sent = up.shape[0] - half * LANES // cells
    edge = HALO * BS
    for g in range(levels // 8):
        q, at = (8 * g) // quarter, (8 * g) % quarter
        a = roll(from_right[at : at + 8, :], -span * q)
        b = roll(from_left[at : at + 8, :], span - span * q)
        side_levels[8 * g : 8 * g + 8, :] = jnp.where(
            lane < span, a, jnp.where(lane < 2 * span, b, 0.0)
        )
    both = jnp.concatenate([fields[...], face0[...]], axis=0)
    full = dot(both, xin[...])
    n = fields.shape[0]
    ext[:, 0:cells] = full[0:n, :]
    q0[...] = full[n : n + 8, :]
    ext[:, cells : cells + LANES] = dot(fields[...], side_levels[...])
    for g in range(half // 8):
        low = side_levels[8 * g : 8 * g + 8, :]
        high = side_levels[half + 8 * g : half + 8 * g + 8, :]
        at, lanes = side_spot(sent, half, cells, 8 * g)
        both = low + roll(high, 2 * span)
        up[at : at + 8, lanes] = both
        dn[at : at + 8, lanes] = both

    @pl.when(jnp.logical_not(ocean))
    def _():
        up[0:sent, :] = xin[0:sent, :]
        dn[0:sent, :] = xin[0:sent, :]

    @pl.when(ocean)
    def _():
        for part in range(2):
            rows_of = slice(part * half, (part + 1) * half)
            lanes_of = slice(part * edge, (part + 1) * edge)
            up[0:half, lanes_of] = xin[rows_of, cells - edge : cells]
            dn[0:half, lanes_of] = xin[rows_of, 0:edge]
        up[half:sent, :] = jnp.zeros((sent - half, cells), F32)
        dn[half:sent, :] = jnp.zeros((sent - half, cells), F32)


def side_spot(sent, half, cells, gs):
    rows = half * LANES // cells
    c, at = divmod(gs, rows)
    return sent + at, slice(c * LANES, (c + 1) * LANES)


def side_lanes(block, at_right, at_left):
    lane = lane_of()
    a = roll(block, -at_right)
    b = roll(block, LANES - RIM - at_left)
    return jnp.where(lane < RIM, a, jnp.where(lane >= LANES - RIM, b, 0.0))


def place_row(x_ref, i, at, blocks, rows):
    span = rows * RIM
    for g, (main, side, shift) in enumerate(blocks):
        x_ref[8 * g : 8 * g + 8, at * WIDE : at * WIDE + LANES] = main
        x_ref[8 * g : 8 * g + 8, at * WIDE + LANES : (at + 1) * WIDE] = side_lanes(
            side, shift + i * RIM, shift + span + i * RIM
        )


def tap_counts(codes, coef, rows, first_row, links):
    count, wide = codes.shape[1], codes.shape[2]
    row = (lax.broadcasted_iota(jnp.int32, (count, wide), 0) + first_row) % rows
    pcol = lax.broadcasted_iota(jnp.int32, (count, wide), 1) % LANES
    width = BS + 2 * HALO
    kinds = []
    for k in range(links):
        n = codes[k].astype(jnp.int32)
        line = ((n.astype(F32) + 0.5) * (1.0 / width)).astype(jnp.int32)
        kinds.append((line - row) * 16 + (n - line * width - pcol))
    for dr in range(TAPS):
        for dc in range(TAPS):
            hits = jnp.zeros((count, wide), F32)
            for k in range(links):
                hits = hits + jnp.where(kinds[k] == dr * 16 + dc, 1.0, 0.0)
            coef[dr * TAPS + dc] = roll(hits, dc - HALO)


def stencil(src, dst, coef, groups, first, count, batch, step=1):
    def row(i):
        off = [pl.multiple_of((i + dr - HALO) * WIDE, WIDE) for dr in range(TAPS)]
        here = pl.multiple_of(i * WIDE, WIDE)
        for g0 in range(0, groups, batch):
            gs = range(g0, min(g0 + batch, groups))
            acc = {}
            for dr in range(TAPS):
                v = {g: src[8 * g : 8 * g + 8, pl.ds(off[dr], WIDE)] for g in gs}
                for dc in range(TAPS):
                    c = coef[dr * TAPS + dc, pl.ds(i, 1), :]
                    for g in gs:
                        t = c * v[g]
                        acc[g, dc] = t if dr == 0 else acc[g, dc] + t
            for g in gs:
                total = acc[g, HALO]
                for dc in range(TAPS):
                    if dc != HALO:
                        total = total + roll(acc[g, dc], HALO - dc)
                dst[8 * g : 8 * g + 8, pl.ds(here, WIDE)] = total

    def one(o, _):
        for p in range(step):
            row(first + o * step + p)
        return 0

    lax.fori_loop(0, count // step, one, 0)


def chain(xa, xb, coef, groups, rows, near, batch, take, step=1):
    total = rows * (2 * near + 1)
    refs = (xa, xb)
    lo = near * rows
    take(0, xa, lo)
    for j in range(1, STEPS + 1):
        src, dst = refs[(j - 1) % 2], refs[j % 2]
        first = lo - RIM + HALO * j
        stencil(src, dst, coef, groups, first, total - 2 * first, batch, step)
        take(j, dst, lo)


def ext_row(block, g, i, rows):
    cells = rows * BS
    main = block[8 * g : 8 * g + 8, i * BS : (i + 1) * BS]
    side = side_lanes(block[8 * g : 8 * g + 8, cells : cells + LANES], i * RIM, (rows + i) * RIM)
    return main, side


def flux_body(rows, near, nf, links, *refs):
    n = 2 * near + 1
    blocks, (mine, q0, cell_in, out, xa, xb, codes, coef, ua, ub, own_codes, own_coef) = (
        refs[:n], refs[n:],
    )
    cells = rows * BS
    groups = nf * STEPS // 8

    @pl.when(lax.axis_index("grp") == 1)
    def _():
        codes[...] = jnp.zeros(codes.shape, F32)
        own_codes[...] = jnp.zeros(own_codes.shape, F32)
        for d in range(n):
            for i in range(rows):
                at = d * rows + i
                for g in range(groups):
                    main, side = ext_row(blocks[d], g, i, rows)
                    xa[8 * g : 8 * g + 8, at * WIDE : at * WIDE + LANES] = main
                    xa[8 * g : 8 * g + 8, at * WIDE + LANES : (at + 1) * WIDE] = side
                main, side = ext_row(blocks[d], groups, i, rows)
                for k in range(links):
                    codes[k, at : at + 1, 0:LANES] = main[nf + k : nf + k + 1, :]
                    codes[k, at : at + 1, LANES:WIDE] = side[nf + k : nf + k + 1, :]
                to = at - near * rows + HALO
                if 0 <= to < rows + 2 * HALO:
                    if d == near:
                        main, side = ext_row(mine, groups, i, rows)
                        for k in range(links):
                            own_codes[k, to : to + 1, 0:LANES] = cell_in[
                                k : k + 1, i * BS : (i + 1) * BS
                            ]
                    ua[:, to * WIDE : to * WIDE + LANES] = main
                    ua[:, to * WIDE + LANES : (to + 1) * WIDE] = side
        tap_counts(own_codes, own_coef, rows, rows - HALO, links)
        stencil(ua, ub, own_coef, 1, HALO, rows, 1, rows)
        tap_counts(codes, coef, rows, 0, links)
        own = blocks[near]
        out[0:nf, :] = own[nf * STEPS : nf * (STEPS + 1), 0:cells]
        for i in range(rows):
            here = slice(i * BS, (i + 1) * BS)
            face = q0[:, here] + ub[:, (HALO + i) * WIDE : (HALO + i) * WIDE + LANES]
            out[nf:8, here] = face[0 : 8 - nf, :]

        def take(j, ref, lo):
            if j == 0:
                return
            at = nf * (j - 1)
            for i in range(rows):
                here = slice(i * BS, (i + 1) * BS)
                out[0:nf, here] = (
                    out[0:nf, here] + ref[at : at + nf, (lo + i) * WIDE : (lo + i) * WIDE + LANES]
                )

        chain(xa, xb, coef, groups, rows, near, groups, take, 4)


def ocean_body(rows, links, sent, xin, cell_in, above, below, own, near, x, y, codes, coef):
    levels, cells = xin.shape
    half, edge = levels // 2, HALO * BS
    groups = levels // 8

    @pl.when(lax.axis_index("grp") == 1)
    def _():
        for at in range(rows + 2 * HALO):
            if at < HALO:
                i, side = rows - HALO + at, above
            elif at < HALO + rows:
                i, side = at - HALO, own
            else:
                i, side = at - HALO - rows, below
            parts = []
            for g in range(groups):
                part, gs = divmod(8 * g, half)
                if at < HALO:
                    main = above[gs : gs + 8, part * edge + at * BS : part * edge + (at + 1) * BS]
                elif at < HALO + rows:
                    main = xin[8 * g : 8 * g + 8, i * BS : (i + 1) * BS]
                else:
                    main = below[gs : gs + 8, part * edge + i * BS : part * edge + (i + 1) * BS]
                s, lanes = side_spot(sent, half, cells, gs)
                parts.append((main, side[s : s + 8, lanes], part * 2 * rows * RIM))
            place_row(x, i, at, parts, rows)
        codes[...] = jnp.zeros(codes.shape, F32)
        for k in range(links):
            for i in range(rows):
                codes[k, HALO + i : HALO + i + 1, 0:LANES] = cell_in[
                    k : k + 1, i * BS : (i + 1) * BS
                ]
        tap_counts(codes, coef, rows, rows - HALO, links)
        stencil(x, y, coef, groups, HALO, rows, 3)
        for i in range(rows):
            near[:, i * BS : (i + 1) * BS] = y[:, (HALO + i) * WIDE : (HALO + i) * WIDE + LANES]


def onto_body(links, cells, count, *refs):
    tables, (high, low, whole) = refs[:count], refs[count:]
    me = lax.axis_index("sub")
    for d in range(count):
        at = pl.multiple_of(((me + d) % count) * cells, cells)
        if tables[d].shape[1] == cells:
            whole[:, pl.ds(at, cells)] = tables[d][...]
        else:
            first = tables[d].shape[0] - 8 * (cells // LANES)
            for c in range(cells // LANES):
                whole[:, pl.ds(pl.multiple_of(at + c * LANES, LANES), LANES)] = tables[d][
                    first + 8 * c : first + 8 * c + 8, :
                ]

    @pl.when(lax.axis_index("grp") == 1)
    def _():
        def chunk(c, _):
            at = pl.multiple_of(c * LANES, LANES)
            src = whole[0:links, pl.ds(at, LANES)].astype(jnp.int32) - me * cells
            w = whole[links : 2 * links, pl.ds(at, LANES)]
            for t in range(0, cells, 16):
                target = lax.broadcasted_iota(jnp.int32, (16, LANES), 0) + t
                value = jnp.zeros((16, LANES), F32)
                for k in range(links):
                    value = value + jnp.where(src[k : k + 1, :] == target, w[k : k + 1, :], 0.0)
                top = value.astype(BF16)
                high[t : t + 16, pl.ds(at, LANES)] = top
                low[t : t + 16, pl.ds(at, LANES)] = (value - top.astype(F32)).astype(BF16)
            return 0

        lax.fori_loop(0, count * cells // LANES, chunk, 0)


def stacked(x, y):
    sub = lax.broadcasted_iota(jnp.int32, x.shape, 0)
    return jnp.where(sub < 4, x, pltpu.roll(y, 4, 0))


def couple_body(links, nf, nr, count, *refs):
    blocks, (whole, high, low, lift, own_flux, out, slab, pair, surface) = (
        refs[:count], refs[count:],
    )
    cells = blocks[0].shape[1]
    levels = lift.shape[0] - 8
    me = lax.axis_index("sub")

    @pl.when(lax.axis_index("grp") == 1)
    def _():
        for d in range(count):
            at = pl.multiple_of(((me + d) % count) * cells, cells)
            block = blocks[d][...]
            slab[:, pl.ds(at, cells)] = block
            pair[:, pl.ds(at, cells)] = stacked(block, block)
        chunks = count * cells // LANES
        half = chunks // 2
        per = min(chunks, 16)
        mine = cells // LANES
        sub = lax.broadcasted_iota(jnp.int32, (8, LANES), 0)

        def two(a, b):
            return jnp.where(sub < 4, a, b)

        def target(c):
            at0 = pl.multiple_of(c * LANES, LANES)
            at1 = pl.multiple_of((c + half) * LANES, LANES)
            t0, t1 = whole[:, pl.ds(at0, LANES)], whole[:, pl.ds(at1, LANES)]
            src, w = [], []
            for k in range(links):
                src.append(two(t0[k : k + 1, :], t1[k : k + 1, :]).astype(jnp.int32))
                w.append(two(t0[links + k : links + k + 1, :], t1[links + k : links + k + 1, :]))
            lanes = [x & (LANES - 1) for x in src]
            homes = [x // LANES for x in src]

            def source(o, acc):
                acc = list(acc)
                for p in range(per):
                    b = o * per + p
                    v = pair[:, pl.ds(pl.multiple_of(b * LANES, LANES), LANES)]
                    for k in range(links):
                        got = jnp.take_along_axis(v, lanes[k], axis=1)
                        acc[k] = jnp.where(homes[k] == b, got, acc[k])
                return tuple(acc)

            zero = tuple(jnp.zeros((8, LANES), F32) for _ in range(links))
            got = source(0, zero) if chunks == per else lax.fori_loop(0, chunks // per, source, zero)
            flux = w[0] * got[0]
            for k in range(1, links):
                flux = flux + w[k] * got[k]
            s0, s1 = slab[:, pl.ds(at0, LANES)], slab[:, pl.ds(at1, LANES)]
            face = stacked(pltpu.roll(s0, 8 - nf, 0), pltpu.roll(s1, 8 - nf, 0))
            col = lift[levels : levels + 8, :]
            col = stacked(col, col)
            for f in range(nf):
                face = face + col[:, f : f + 1] * two(flux[f : f + 1, :], flux[4 + f : 5 + f, :])
            n = 2 * links
            face = jnp.where(
                sub % 4 < nr, face * two(t0[n : n + 1, :], t1[n : n + 1, :]), 0.0
            )
            surface[:, pl.ds(at0, LANES)] = face
            for part, lift_rows in ((0, flux), (1, pltpu.roll(flux, 4, 0))):
                here = c + part * half - me * mine

                @pl.when((here >= 0) & (here < mine))
                def _():
                    own_flux[:, pl.ds(pl.multiple_of(here * LANES, LANES), LANES)] = jnp.where(
                        sub < nf, lift_rows, 0.0
                    )

        def some(o, _):
            for p in range(2):
                target(o * 2 + p)
            return 0

        lax.fori_loop(0, half // 2, some, 0)
        face = surface[...]
        top = face.astype(BF16)
        rest = (face - top.astype(F32)).astype(BF16)
        both = jnp.concatenate([top, rest], axis=0)

        def nt(a, b):
            return lax.dot_general(a, b, (((1,), (1,)), ((), ())), preferred_element_type=F32)

        cut = half * LANES
        one = nt(both, high[:, 0:cut])
        two_ = nt(top, low[:, 0:cut])
        three = nt(both, high[:, cut : 2 * cut])
        four = nt(top, low[:, cut : 2 * cut])
        first = one[0:8, :] + one[8:16, :] + two_
        second = three[0:8, :] + three[8:16, :] + four
        out[...] = first + pltpu.roll(second, 4, 0)


def place_blocks(x, codes, blocks, spots, sent, half, links):
    rows = blocks[0].shape[1] // BS
    for block, at0 in zip(blocks, spots):
        for i in range(rows):
            parts = []
            for g in range(sent // 8):
                part, gs = divmod(8 * g, half)
                s, lanes = side_spot(sent, half, block.shape[1], gs)
                parts.append(
                    (
                        block[8 * g : 8 * g + 8, i * BS : (i + 1) * BS],
                        block[s : s + 8, lanes],
                        part * 2 * rows * RIM,
                    )
                )
            at = at0 + i
            place_row(x, i, at, parts, rows)
            for k in range(links):
                s = LA + k
                codes[k, at : at + 1, :] = x[s : s + 1, at * WIDE : (at + 1) * WIDE]


def inner_body(rows, links, sent, levels, above, own, below, x0, x1, x2, codes, coef):
    groups = sent // 8
    total = 3 * rows

    @pl.when(lax.axis_index("grp") == 0)
    def _():
        codes[...] = jnp.zeros(codes.shape, F32)
        place_blocks(
            x0, codes, (above, own, below), (0, rows, 2 * rows), sent, levels // 2, links
        )
        tap_counts(codes, coef, rows, 0, links)
        stencil(x0, x1, coef, groups, HALO, total - 2 * HALO, 3)
        stencil(x1, x2, coef, groups, 2 * HALO, total - 4 * HALO, 3)


def state_body(rows, links, sent, far_up, far_dn, x0_in, x1_in, x2_in, powers, xin, near_sum,
               own_mix, own_flux, lift, table, out, x0, x1, x2, x3, codes, coef, basis):
    levels, cells = out.shape
    groups = sent // 8
    total = 5 * rows
    ocean = lax.axis_index("grp") == 1

    @pl.when(ocean)
    def _():
        start = xin[...]
        now = (
            dot(own_mix[:, 0:levels], start)
            + dot(own_mix[:, levels:], near_sum[...])
            + dot(lift[0:levels, :], own_flux[...])
        )
        wet = table[2 * links : 2 * links + 1, :]
        out[...] = start + wet * (now - start)

    @pl.when(jnp.logical_not(ocean))
    def _():
        codes[...] = jnp.zeros(codes.shape, F32)
        for j, (ref, given) in enumerate(((x0, x0_in), (x1, x1_in), (x2, x2_in))):
            lo, hi = HALO * j, 3 * rows - HALO * j
            ref[:, (rows + lo) * WIDE : (rows + hi) * WIDE] = given[:, lo * WIDE : hi * WIDE]
        place_blocks(
            x0, codes, (far_up, far_dn), (0, 4 * rows), sent, levels // 2, links
        )
        for at in range(rows, 4 * rows):
            for k in range(links):
                s = LA + k
                codes[k, at : at + 1, :] = x0[s : s + 1, at * WIDE : (at + 1) * WIDE]
        tap_counts(codes, coef, rows, 0, links)

        def apply(src, dst, j, done=None):
            lo, hi = HALO * j, total - HALO * j
            if done is None:
                stencil(src, dst, coef, groups, lo, hi - lo, 3)
                return
            stencil(src, dst, coef, groups, lo, done[0] - lo, 3)
            stencil(src, dst, coef, groups, done[1], hi - done[1], 3)

        apply(x0, x1, 1, (rows + HALO, 4 * rows - HALO))
        apply(x1, x2, 2, (rows + 2 * HALO, 4 * rows - 2 * HALO))
        apply(x2, x3, 3)
        basis[...] = jnp.zeros(basis.shape, F32)
        mid = 2 * rows

        def take(j, ref):
            for i in range(rows):
                basis[j * levels : j * levels + sent, i * BS : (i + 1) * BS] = ref[
                    0:sent, (mid + i) * WIDE : (mid + i) * WIDE + LANES
                ]

        for j, ref in enumerate((x0, x1, x2, x3)):
            take(j, ref)
        apply(x3, x0, 4)
        take(4, x0)
        out[0:sent, :] = dot(powers[...], basis[...])
        if sent < levels:
            out[sent:levels, :] = jnp.zeros((levels - sent, cells), F32)


def local(
    column_state,
    neighbours,
    mixing,
    diffusivity,
    flux_map,
    force_map,
    return_map,
    sources,
    remap_weights,
    wet,
):
    levels, cells = column_state.shape[1:]
    rows = cells // BS
    links = neighbours.shape[1]
    nf, nr = flux_map.shape[0], return_map.shape[0]
    near = -(-RIM // rows)
    n = 2 * near + 1
    sent = max(up8(LA + links), levels // 2)
    n_reg, n_sub = lax.axis_size("reg"), lax.axis_size("sub")
    axes = ("grp", "reg", "sub")

    def at(g, r, s):
        return (g * n_reg + r % n_reg) * n_sub + s % n_sub

    spots = [(r, s) for r in range(n_reg) for s in range(n_sub)]

    def shift(x, axis, d):
        size = lax.axis_size(axis)
        return lax.ppermute(x, axis, [((i + d) % size, i) for i in range(size)])

    def stack_rows(parts, count):
        out, at = None, 0
        for p in parts:
            here = jnp.pad(p, ((at, up8(count) - at - p.shape[0]), (0, 0)))
            at += p.shape[0]
            out = here if out is None else out + here
        return out

    whole_numbers = stack_rows(
        [neighbours[0], sources, jnp.zeros((links, cells), jnp.int32), wet[None]], 3 * links + 2
    )
    cell_in = whole_numbers.astype(F32) + jnp.pad(
        remap_weights, ((2 * links, up8(3 * links + 2) - 3 * links), (0, 0))
    )
    small = stack_rows([diffusivity, flux_map, force_map.T, return_map], 1 + 2 * nf + nr)
    ext_rows = up8(nf * (STEPS + 1) + links)
    message = levels // 4 + 8 * (cells // LANES)
    xin, to_left, to_right, table = call(
        functools.partial(pack_body, links),
        (
            shape(levels, cells),
            shape(message, LANES),
            shape(message, LANES),
            shape(8, cells),
        ),
        column_state[0], cell_in,
        vmem=8 << 20,
    )
    from_right = shift(to_left, "sub", 1)
    from_left = shift(to_right, "sub", -1)
    fields, face0 = call(
        functools.partial(fields_body, nf, nr, links),
        (shape(ext_rows, levels), shape(8, levels)),
        mixing[0], small,
        vmem=8 << 20,
    )
    powers, own_mix, lift = call(
        functools.partial(powers_body, nf, nr, links),
        (
            shape(sent, (STEPS + 1) * levels),
            shape(levels, 2 * levels),
            shape(levels + 8, 8),
        ),
        mixing[0], small,
        vmem=8 << 20,
    )
    block = sent + levels // 2 * LANES // cells
    up, dn, ext, q0 = call(
        side_body,
        (
            shape(block, cells),
            shape(block, cells),
            shape(ext_rows, cells + LANES),
            shape(8, cells),
        ),
        xin, from_right, from_left, fields, face0,
        scratch=[pltpu.VMEM((levels, LANES), F32)],
        vmem=8 << 20,
    )

    hop = lax.ppermute(ext, axes, [(at(0, r, s), at(1, r, s)) for r, s in spots])
    line = lax.broadcasted_iota(jnp.int32, ext.shape, 0)
    relay = jnp.where((line >= nf * STEPS) & (line < nf * (STEPS + 1)), ext, hop)
    got, mains = {0: hop}, {}
    for d in sorted(range(-near, near + 1), key=abs):
        key = d % n_reg
        if key in got:
            continue
        pairs = [(at(1, r + d, s), at(1, r, s)) for r, s in spots]
        got[key] = lax.ppermute(relay, axes, pairs)
        groups = (0, 1) if abs(d) == 1 else (0,)
        pairs = [(at(g, r + d, s), at(g, r, s)) for g in groups for r, s in spots]
        mains[key] = lax.ppermute(up if d < 0 else dn, axes, pairs)
    ext_blocks = [got[d % n_reg] for d in range(-near, near + 1)]
    above, below = mains[-1 % n_reg], mains[1 % n_reg]

    tables = [table] + [None] * (n_sub - 1)
    tables[1], tables[n_sub - 1] = from_right, from_left
    for d in range(2, n_sub - 1):
        tables[d] = shift(table, "sub", d)
    span = n_sub * cells
    high, low, whole = call(
        functools.partial(onto_body, links, cells, n_sub),
        (shape(cells, span, dtype=BF16), shape(cells, span, dtype=BF16), shape(8, span)),
        *tables,
        vmem=24 << 20,
    )

    ext_o = up8(rows + 2 * HALO)
    near_sum = call(
        functools.partial(ocean_body, rows, links, sent),
        shape(levels, cells),
        xin, cell_in, above, below, up,
        scratch=[
            pltpu.VMEM((levels, (rows + 2 * HALO) * WIDE), F32),
            pltpu.VMEM((levels, (rows + 2 * HALO) * WIDE), F32),
            pltpu.VMEM((links, ext_o, WIDE), F32),
            pltpu.VMEM((TAPS * TAPS, ext_o, WIDE), F32),
        ],
        vmem=16 << 20,
    )

    total = rows * n
    ext_n = up8(total)
    fq = call(
        functools.partial(flux_body, rows, near, nf, links),
        shape(8, cells),
        *ext_blocks, ext, q0, cell_in,
        scratch=[
            pltpu.VMEM((nf * STEPS, total * WIDE), F32),
            pltpu.VMEM((nf * STEPS, total * WIDE), F32),
            pltpu.VMEM((links, ext_n, WIDE), F32),
            pltpu.VMEM((TAPS * TAPS, ext_n, WIDE), F32),
            pltpu.VMEM((8, (rows + 2 * HALO) * WIDE), F32),
            pltpu.VMEM((8, (rows + 2 * HALO) * WIDE), F32),
            pltpu.VMEM((links, ext_o, WIDE), F32),
            pltpu.VMEM((TAPS * TAPS, ext_o, WIDE), F32),
        ],
        vmem=8 << 20,
    )
    blocks = [fq] + [shift(fq, "sub", d) for d in range(1, n_sub)]
    own_flux, coupled = call(
        functools.partial(couple_body, links, nf, nr, n_sub),
        (shape(8, cells), shape(8, cells)),
        *blocks, whole, high, low, lift,
        scratch=[
            pltpu.VMEM((8, span), F32),
            pltpu.VMEM((8, span), F32),
            pltpu.VMEM((8, span // 2), F32),
        ],
        vmem=24 << 20,
    )
    back = lax.ppermute(coupled, axes, [(at(1, r, s), at(0, r, s)) for r, s in spots])

    wide = 3 * rows * WIDE
    ext_i = up8(3 * rows)
    x0, x1, x2 = call(
        functools.partial(inner_body, rows, links, sent, levels),
        (shape(sent, wide), shape(sent, wide), shape(sent, wide)),
        above, up, below,
        scratch=[
            pltpu.VMEM((links, ext_i, WIDE), F32),
            pltpu.VMEM((TAPS * TAPS, ext_i, WIDE), F32),
        ],
        vmem=12 << 20,
    )
    new_state = call(
        functools.partial(state_body, rows, links, sent),
        shape(levels, cells),
        mains[-2 % n_reg], mains[2 % n_reg], x0, x1, x2, powers, xin, near_sum, own_mix, own_flux,
        lift, table,
        scratch=[pltpu.VMEM((sent, total * WIDE), F32) for _ in range(4)]
        + [
            pltpu.VMEM((links, ext_n, WIDE), F32),
            pltpu.VMEM((TAPS * TAPS, ext_n, WIDE), F32),
            pltpu.VMEM(((STEPS + 1) * levels, cells), F32),
        ],
        vmem=24 << 20,
    )
    ocean_side = lax.axis_index("grp") == 1
    surface = jnp.where(ocean_side, coupled[:nr], back[:nr])
    return (new_state[None], surface)


def solution(mesh):
    in_specs = (
        P("grp", None, ("reg", "sub")),
        P("grp", None, ("reg", "sub")),
        P("grp", None, None),
        P("grp", None),
        P(),
        P(),
        P(),
        P(None, ("reg", "sub")),
        P(None, ("reg", "sub")),
        P(("reg", "sub")),
    )
    out_specs = (P("grp", None, ("reg", "sub")), P(None, ("reg", "sub")))
    return jax.shard_map(local, mesh=mesh, in_specs=in_specs, out_specs=out_specs, check_vma=False)
```

```python
import functools
import jax
import jax.numpy as jnp
from jax import lax
from jax.experimental import pallas as pl
from jax.experimental.pallas import tpu as pltpu
from jax.sharding import PartitionSpec as P

LA = 90
BS = 128
HALO = 2
STEPS = 4
RIM = HALO * STEPS
TAPS = 2 * HALO + 1
HIGH = lax.Precision.HIGHEST
F32 = jnp.float32
BF16 = jnp.bfloat16
LANES = 128
WIDE = 2 * LANES


def up8(n):
    return -(-n // 8) * 8


def dot(a, b):
    return jnp.dot(a, b, precision=HIGH, preferred_element_type=F32)


def lane_of(width=LANES, rows=8):
    return lax.broadcasted_iota(jnp.int32, (rows, width), 1)


def roll(x, shift):
    shift = shift % x.shape[1]
    return x if shift == 0 else pltpu.roll(x, shift, 1)


def call(body, outs, *args, scratch=(), vmem=None, flops=100000, alias=None):
    size = sum(a.size * a.dtype.itemsize for a in args)
    return pl.pallas_call(
        body,
        out_shape=outs,
        in_specs=[pl.BlockSpec(memory_space=pltpu.VMEM) for _ in args],
        out_specs=jax.tree.map(lambda _: pl.BlockSpec(memory_space=pltpu.VMEM), outs),
        scratch_shapes=list(scratch),
        input_output_aliases=alias or {},
        compiler_params=pltpu.CompilerParams(vmem_limit_bytes=vmem),
        cost_estimate=pl.CostEstimate(flops=flops, bytes_accessed=size, transcendentals=0),
    )(*args)


def shape(*dims, dtype=F32):
    return jax.ShapeDtypeStruct(dims, dtype)


def pack_body(links, state, cell_in, xin, to_left, to_right, table):
    levels, cells = xin.shape
    rows = cells // BS
    ocean = lax.axis_index("grp") == 1

    @pl.when(jnp.logical_not(ocean))
    def _():
        level = lax.broadcasted_iota(jnp.int32, (levels, cells), 0)
        xin[...] = jnp.where(level < LA, state[...], 0.0)
        xin[LA : LA + links, :] = cell_in[0:links, :]

    @pl.when(ocean)
    def _():
        xin[...] = state[...]

    lane = lane_of()
    quarter = levels // 4
    span = rows * RIM
    for g in range(quarter // 8):
        left = jnp.zeros((8, LANES), F32)
        right = jnp.zeros((8, LANES), F32)
        for q in range(4):
            for i in range(rows):
                at = q * span + i * RIM
                here = (lane >= at) & (lane < at + RIM)
                block = xin[q * quarter + 8 * g : q * quarter + 8 * g + 8, i * BS : (i + 1) * BS]
                left = jnp.where(here, roll(block, at), left)
                right = jnp.where(here, roll(block, at - (BS - RIM)), right)
        to_left[8 * g : 8 * g + 8, :] = left
        to_right[8 * g : 8 * g + 8, :] = right
    table[...] = cell_in[links : links + 8, :]
    for c in range(cells // LANES):
        part = table[:, c * LANES : (c + 1) * LANES]
        to_left[quarter + 8 * c : quarter + 8 * c + 8, :] = part
        to_right[quarter + 8 * c : quarter + 8 * c + 8, :] = part


def level_matrix(mixing):
    levels = mixing.shape[0]
    row = lax.broadcasted_iota(jnp.int32, (levels, levels), 0)
    col = lax.broadcasted_iota(jnp.int32, (levels, levels), 1)
    full = mixing[...] + jnp.where(row == col, 1.0, 0.0)
    return full, jnp.where((row < LA) & (col < LA), full, 0.0)


def fields_body(nf, nr, links, mixing, small, fields, face0):
    levels = mixing.shape[0]
    full, base = level_matrix(mixing)
    r = small[0:1, :]
    ocean = lax.axis_index("grp") == 1
    at = nf * STEPS
    fields[...] = jnp.zeros(fields.shape, F32)

    @pl.when(jnp.logical_not(ocean))
    def _():
        pair = jnp.concatenate([base * (1.0 - float(links) * r), base * r], axis=1)
        lead = jnp.concatenate([small[1 : 1 + nf, :], jnp.zeros((8 - nf, levels), F32)], axis=0)
        have = [lead]
        total = [jnp.zeros((8, levels), F32) for _ in range(STEPS + 1)]
        for n in range(1, STEPS + 1):
            out = dot(jnp.concatenate(have, axis=0) if len(have) > 1 else have[0], pair)
            new = []
            for j in range(n + 1):
                term = jnp.zeros((8, levels), F32)
                if j < n:
                    term = term + out[8 * j : 8 * j + 8, :levels]
                if j > 0:
                    term = term + out[8 * j - 8 : 8 * j, levels:]
                new.append(term)
                total[j] = total[j] + term
            have = new
        for j in range(STEPS + 1):
            to = nf * ((j - 1) % (STEPS + 1))
            fields[to : to + nf, :] = total[j][0:nf, :] * (1.0 / STEPS)
        k = lax.broadcasted_iota(jnp.int32, (links, levels), 0)
        c = lax.broadcasted_iota(jnp.int32, (links, levels), 1)
        fields[at + nf : at + nf + links, :] = jnp.where(c == LA + k, 1.0, 0.0)
        face0[...] = jnp.zeros(face0.shape, F32)

    @pl.when(ocean)
    def _():
        first = 1 + 2 * nf
        lead = jnp.concatenate(
            [small[first : first + nr, :], jnp.zeros((8 - nr, levels), F32)], axis=0
        )
        through = dot(lead, full)
        face0[...] = through * (1.0 - float(links) * r)
        fields[at : at + nr, :] = (through * r)[0:nr, :]


def powers_body(nf, nr, links, sent, mixing, small, powers, own_mix, lift):
    levels = mixing.shape[0]
    full, base = level_matrix(mixing)
    r = small[0:1, :]
    ocean = lax.axis_index("grp") == 1

    @pl.when(jnp.logical_not(ocean))
    def _():
        def squared(mats):
            n = len(mats)
            prod = dot(jnp.concatenate(mats, axis=0), jnp.concatenate(mats, axis=1))
            outs = []
            for j in range(2 * n - 1):
                term = None
                for a in range(n):
                    b = j - a
                    if 0 <= b < n:
                        piece = prod[a * levels : (a + 1) * levels, b * levels : (b + 1) * levels]
                        term = piece if term is None else term + piece
                outs.append(term)
            return outs

        mats = squared(squared([base * (1.0 - float(links) * r), base * r]))
        wide = powers.shape[1]
        whole = jnp.zeros((sent, wide), F32)
        for j in range(STEPS + 1):
            part = jnp.concatenate(
                [mats[j][0:sent, :], jnp.zeros((sent, wide - levels), F32)], axis=1
            )
            whole = whole + roll(part, j * sent)
        top = whole.astype(BF16)
        powers[0:sent, :] = top
        powers[sent : 2 * sent, :] = (whole - top.astype(F32)).astype(BF16)

    @pl.when(ocean)
    def _():
        own_mix[:, 0:levels] = full * (1.0 - float(links) * r)
        own_mix[:, levels : 2 * levels] = full * r
        first = 1 + 2 * nf
        lead = jnp.concatenate(
            [small[first : first + nr, :], jnp.zeros((8 - nr, levels), F32)], axis=0
        )
        top = jnp.concatenate(
            [small[1 + nf : 1 + 2 * nf, :], jnp.zeros((8 - nf, levels), F32)], axis=0
        )
        lifted = lax.dot_general(
            full, top, (((1,), (1,)), ((), ())), precision=HIGH, preferred_element_type=F32
        )
        lift[0:levels, :] = lifted
        lift[levels : levels + 8, :] = dot(lead, lifted)


def side_body(xin, from_right, from_left, fields, face0, up, dn, far, ext, q0, extra, side_levels):
    levels, cells = xin.shape
    rows = cells // BS
    quarter, half = levels // 4, levels // 2
    span = rows * RIM
    lane = lane_of()
    ocean = lax.axis_index("grp") == 1
    sent = up.shape[0]
    edge = HALO * BS
    for g in range(levels // 8):
        q, at = (8 * g) // quarter, (8 * g) % quarter
        a = roll(from_right[at : at + 8, :], -span * q)
        b = roll(from_left[at : at + 8, :], span - span * q)
        side_levels[8 * g : 8 * g + 8, :] = jnp.where(
            lane < span, a, jnp.where(lane < 2 * span, b, 0.0)
        )
    both = jnp.concatenate([fields[...], face0[...]], axis=0)
    full = dot(both, xin[...])
    n = fields.shape[0]
    ext[:, 0:cells] = full[0:n, :]
    q0[...] = full[n : n + 8, :]
    ext[:, cells : cells + LANES] = dot(fields[...], side_levels[...])
    for g in range(half // 8):
        low = side_levels[8 * g : 8 * g + 8, :]
        high = side_levels[half + 8 * g : half + 8 * g + 8, :]
        both = low + roll(high, 2 * span)
        at, lanes = side_spot(0, half, cells, 8 * g)
        extra[at : at + 8, lanes] = both

    n = half * LANES // cells
    more = extra.shape[0] - n
    extra[n:, 0:cells] = xin[sent : sent + more, :]
    extra[:, cells:] = jnp.zeros((n + more, LANES), F32)

    @pl.when(jnp.logical_not(ocean))
    def _():
        up[...] = xin[0:sent, :]
        dn[...] = xin[0:sent, :]
        far[0:sent, :] = xin[0:sent, :]
        far[sent:, :] = extra[:, 0:cells]

    @pl.when(ocean)
    def _():
        for part in range(2):
            rows_of = slice(part * half, (part + 1) * half)
            lanes_of = slice(part * edge, (part + 1) * edge)
            up[0:half, lanes_of] = xin[rows_of, cells - edge : cells]
            dn[0:half, lanes_of] = xin[rows_of, 0:edge]
        for ref in (up, dn):
            ref[half : half + n, :] = extra[0:n, 0:cells]
            ref[half + n :, :] = jnp.zeros((sent - half - n, cells), F32)


def side_spot(sent, half, cells, gs):
    rows = half * LANES // cells
    c, at = divmod(gs, rows)
    return sent + at, slice(c * LANES, (c + 1) * LANES)


def side_lanes(block, at_right, at_left):
    lane = lane_of()
    a = roll(block, -at_right)
    b = roll(block, LANES - RIM - at_left)
    return jnp.where(lane < RIM, a, jnp.where(lane >= LANES - RIM, b, 0.0))


def place_row(x_ref, i, at, blocks, rows):
    span = rows * RIM
    for g, (main, side, shift) in enumerate(blocks):
        x_ref[8 * g : 8 * g + 8, at * WIDE : at * WIDE + LANES] = main
        x_ref[8 * g : 8 * g + 8, at * WIDE + LANES : (at + 1) * WIDE] = side_lanes(
            side, shift + i * RIM, shift + span + i * RIM
        )


def tap_counts(codes, coef, rows, first_row, links, at=0, count=None):
    count, wide = count or codes.shape[1], codes.shape[2]
    row = (lax.broadcasted_iota(jnp.int32, (count, wide), 0) + first_row) % rows
    pcol = lax.broadcasted_iota(jnp.int32, (count, wide), 1) % LANES
    width = BS + 2 * HALO
    kinds = []
    for k in range(links):
        n = codes[k, at : at + count, :].astype(jnp.int32)
        line = ((n.astype(F32) + 0.5) * (1.0 / width)).astype(jnp.int32)
        kinds.append((line - row) * 16 + (n - line * width - pcol))
    for dr in range(TAPS):
        for dc in range(TAPS):
            hits = jnp.zeros((count, wide), F32)
            for k in range(links):
                hits = hits + jnp.where(kinds[k] == dr * 16 + dc, 1.0, 0.0)
            coef[dr * TAPS + dc, at : at + count, :] = roll(hits, dc - HALO)


def same(i):
    return i


def stencil(src, dst, coef, groups, first, count, batch, step=1, slot=same):
    def row(i):
        off = [pl.multiple_of((i + dr - HALO) * WIDE, WIDE) for dr in range(TAPS)]
        here = pl.multiple_of(i * WIDE, WIDE)
        for g0 in range(0, groups, batch):
            gs = range(g0, min(g0 + batch, groups))
            acc = {}
            for dr in range(TAPS):
                v = {g: src[8 * g : 8 * g + 8, pl.ds(off[dr], WIDE)] for g in gs}
                for dc in range(TAPS):
                    c = coef[dr * TAPS + dc, pl.ds(slot(i), 1), :]
                    for g in gs:
                        t = c * v[g]
                        acc[g, dc] = t if dr == 0 else acc[g, dc] + t
            for g in gs:
                total = acc[g, HALO]
                for dc in range(TAPS):
                    if dc != HALO:
                        total = total + roll(acc[g, dc], HALO - dc)
                dst[8 * g : 8 * g + 8, pl.ds(here, WIDE)] = total

    def one(o, _):
        for p in range(step):
            row(first + o * step + p)
        return 0

    lax.fori_loop(0, count // step, one, 0)


def chain(xa, xb, coef, groups, rows, near, batch, take, step=1):
    total = rows * (2 * near + 1)
    refs = (xa, xb)
    lo = near * rows
    take(0, xa, lo)
    for j in range(1, STEPS + 1):
        src, dst = refs[(j - 1) % 2], refs[j % 2]
        first = lo - RIM + HALO * j
        stencil(src, dst, coef, groups, first, total - 2 * first, batch, step)
        take(j, dst, lo)


def ext_row(block, g, i, rows):
    cells = rows * BS
    main = block[8 * g : 8 * g + 8, i * BS : (i + 1) * BS]
    side = side_lanes(block[8 * g : 8 * g + 8, cells : cells + LANES], i * RIM, (rows + i) * RIM)
    return main, side


def flux_body(rows, near, nf, links, *refs):
    n = 2 * near + 1
    blocks, (mine, q0, cell_in, out, xa, xb, codes, coef, ua, ub, own_codes, own_coef) = (
        refs[:n], refs[n:],
    )
    cells = rows * BS
    groups = nf * STEPS // 8

    @pl.when(lax.axis_index("grp") == 1)
    def _():
        codes[...] = jnp.zeros(codes.shape, F32)
        own_codes[...] = jnp.zeros(own_codes.shape, F32)
        for d in range(n):
            for i in range(rows):
                at = d * rows + i
                for g in range(groups):
                    main, side = ext_row(blocks[d], g, i, rows)
                    xa[8 * g : 8 * g + 8, at * WIDE : at * WIDE + LANES] = main
                    xa[8 * g : 8 * g + 8, at * WIDE + LANES : (at + 1) * WIDE] = side
                main, side = ext_row(blocks[d], groups, i, rows)
                for k in range(links):
                    codes[k, at : at + 1, 0:LANES] = main[nf + k : nf + k + 1, :]
                    codes[k, at : at + 1, LANES:WIDE] = side[nf + k : nf + k + 1, :]
                to = at - near * rows + HALO
                if 0 <= to < rows + 2 * HALO:
                    if d == near:
                        main, side = ext_row(mine, groups, i, rows)
                        for k in range(links):
                            own_codes[k, to : to + 1, 0:LANES] = cell_in[
                                k : k + 1, i * BS : (i + 1) * BS
                            ]
                    ua[:, to * WIDE : to * WIDE + LANES] = main
                    ua[:, to * WIDE + LANES : (to + 1) * WIDE] = side
        tap_counts(own_codes, own_coef, rows, rows - HALO, links)
        stencil(ua, ub, own_coef, 1, HALO, rows, 1, rows)
        tap_counts(codes, coef, rows, 0, links)
        own = blocks[near]
        out[0:nf, :] = own[nf * STEPS : nf * (STEPS + 1), 0:cells]
        for i in range(rows):
            here = slice(i * BS, (i + 1) * BS)
            face = q0[:, here] + ub[:, (HALO + i) * WIDE : (HALO + i) * WIDE + LANES]
            out[nf:8, here] = face[0 : 8 - nf, :]

        def take(j, ref, lo):
            if j == 0:
                return
            at = nf * (j - 1)
            for i in range(rows):
                here = slice(i * BS, (i + 1) * BS)
                out[0:nf, here] = (
                    out[0:nf, here] + ref[at : at + nf, (lo + i) * WIDE : (lo + i) * WIDE + LANES]
                )

        chain(xa, xb, coef, groups, rows, near, groups, take, 4)


def ocean_body(rows, links, xin, cell_in, above, below, own, near, x, y, codes, coef):
    levels, cells = xin.shape
    half, edge = levels // 2, HALO * BS
    groups = levels // 8

    @pl.when(lax.axis_index("grp") == 1)
    def _():
        for at in range(rows + 2 * HALO):
            if at < HALO:
                i, side = rows - HALO + at, above
            elif at < HALO + rows:
                i, side = at - HALO, own
            else:
                i, side = at - HALO - rows, below
            parts = []
            for g in range(groups):
                part, gs = divmod(8 * g, half)
                if at < HALO:
                    main = above[gs : gs + 8, part * edge + at * BS : part * edge + (at + 1) * BS]
                elif at < HALO + rows:
                    main = xin[8 * g : 8 * g + 8, i * BS : (i + 1) * BS]
                else:
                    main = below[gs : gs + 8, part * edge + i * BS : part * edge + (i + 1) * BS]
                s, lanes = side_spot(half, half, cells, gs)
                parts.append((main, side[s : s + 8, lanes], part * 2 * rows * RIM))
            place_row(x, i, at, parts, rows)
        codes[...] = jnp.zeros(codes.shape, F32)
        for k in range(links):
            for i in range(rows):
                codes[k, HALO + i : HALO + i + 1, 0:LANES] = cell_in[
                    k : k + 1, i * BS : (i + 1) * BS
                ]
        tap_counts(codes, coef, rows, rows - HALO, links)
        stencil(x, y, coef, groups, HALO, rows, 3)
        for i in range(rows):
            near[:, i * BS : (i + 1) * BS] = y[:, (HALO + i) * WIDE : (HALO + i) * WIDE + LANES]


def onto_body(links, cells, count, *refs):
    tables, (high, low, whole) = refs[:count], refs[count:]
    me = lax.axis_index("sub")
    for d in range(count):
        at = pl.multiple_of(((me + d) % count) * cells, cells)
        if tables[d].shape[1] == cells:
            whole[:, pl.ds(at, cells)] = tables[d][...]
        else:
            first = tables[d].shape[0] - 8 * (cells // LANES)
            for c in range(cells // LANES):
                whole[:, pl.ds(pl.multiple_of(at + c * LANES, LANES), LANES)] = tables[d][
                    first + 8 * c : first + 8 * c + 8, :
                ]

    @pl.when(lax.axis_index("grp") == 1)
    def _():
        def chunk(c, _):
            at = pl.multiple_of(c * LANES, LANES)
            src = whole[0:links, pl.ds(at, LANES)].astype(jnp.int32) - me * cells
            w = whole[links : 2 * links, pl.ds(at, LANES)]
            for t in range(0, cells, 16):
                target = lax.broadcasted_iota(jnp.int32, (16, LANES), 0) + t
                value = jnp.zeros((16, LANES), F32)
                for k in range(links):
                    value = value + jnp.where(src[k : k + 1, :] == target, w[k : k + 1, :], 0.0)
                top = value.astype(BF16)
                high[t : t + 16, pl.ds(at, LANES)] = top
                low[t : t + 16, pl.ds(at, LANES)] = (value - top.astype(F32)).astype(BF16)
            return 0

        lax.fori_loop(0, count * cells // LANES, chunk, 0)


def stacked(x, y):
    sub = lax.broadcasted_iota(jnp.int32, x.shape, 0)
    return jnp.where(sub < 4, x, pltpu.roll(y, 4, 0))


def couple_body(links, nf, nr, count, *refs):
    blocks, (whole, high, low, lift, own_flux, out, slab, pair, surface) = (
        refs[:count], refs[count:],
    )
    cells = blocks[0].shape[1]
    levels = lift.shape[0] - 8
    me = lax.axis_index("sub")

    @pl.when(lax.axis_index("grp") == 1)
    def _():
        for d in range(count):
            at = pl.multiple_of(((me + d) % count) * cells, cells)
            block = blocks[d][...]
            slab[:, pl.ds(at, cells)] = block
            pair[:, pl.ds(at, cells)] = stacked(block, block)
        chunks = count * cells // LANES
        half = chunks // 2
        per = min(chunks, 16)
        mine = cells // LANES
        sub = lax.broadcasted_iota(jnp.int32, (8, LANES), 0)

        def two(a, b):
            return jnp.where(sub < 4, a, b)

        def target(c):
            at0 = pl.multiple_of(c * LANES, LANES)
            at1 = pl.multiple_of((c + half) * LANES, LANES)
            t0, t1 = whole[:, pl.ds(at0, LANES)], whole[:, pl.ds(at1, LANES)]
            src, w = [], []
            for k in range(links):
                src.append(two(t0[k : k + 1, :], t1[k : k + 1, :]).astype(jnp.int32))
                w.append(two(t0[links + k : links + k + 1, :], t1[links + k : links + k + 1, :]))
            lanes = [x & (LANES - 1) for x in src]
            homes = [x // LANES for x in src]

            def source(o, acc):
                acc = list(acc)
                for p in range(per):
                    b = o * per + p
                    v = pair[:, pl.ds(pl.multiple_of(b * LANES, LANES), LANES)]
                    for k in range(links):
                        got = jnp.take_along_axis(v, lanes[k], axis=1)
                        acc[k] = jnp.where(homes[k] == b, got, acc[k])
                return tuple(acc)

            zero = tuple(jnp.zeros((8, LANES), F32) for _ in range(links))
            got = source(0, zero) if chunks == per else lax.fori_loop(0, chunks // per, source, zero)
            flux = w[0] * got[0]
            for k in range(1, links):
                flux = flux + w[k] * got[k]
            s0, s1 = slab[:, pl.ds(at0, LANES)], slab[:, pl.ds(at1, LANES)]
            face = stacked(pltpu.roll(s0, 8 - nf, 0), pltpu.roll(s1, 8 - nf, 0))
            col = lift[levels : levels + 8, :]
            col = stacked(col, col)
            for f in range(nf):
                face = face + col[:, f : f + 1] * two(flux[f : f + 1, :], flux[4 + f : 5 + f, :])
            n = 2 * links
            face = jnp.where(
                sub % 4 < nr, face * two(t0[n : n + 1, :], t1[n : n + 1, :]), 0.0
            )
            surface[:, pl.ds(at0, LANES)] = face
            for part, lift_rows in ((0, flux), (1, pltpu.roll(flux, 4, 0))):
                here = c + part * half - me * mine

                @pl.when((here >= 0) & (here < mine))
                def _():
                    own_flux[:, pl.ds(pl.multiple_of(here * LANES, LANES), LANES)] = jnp.where(
                        sub < nf, lift_rows, 0.0
                    )

        def some(o, _):
            for p in range(2):
                target(o * 2 + p)
            return 0

        lax.fori_loop(0, half // 2, some, 0)
        face = surface[...]
        top = face.astype(BF16)
        rest = (face - top.astype(F32)).astype(BF16)
        both = jnp.concatenate([top, rest], axis=0)

        def nt(a, b):
            return lax.dot_general(a, b, (((1,), (1,)), ((), ())), preferred_element_type=F32)

        cut = half * LANES
        one = nt(both, high[:, 0:cut])
        two_ = nt(top, low[:, 0:cut])
        three = nt(both, high[:, cut : 2 * cut])
        four = nt(top, low[:, cut : 2 * cut])
        first = one[0:8, :] + one[8:16, :] + two_
        second = three[0:8, :] + three[8:16, :] + four
        out[...] = first + pltpu.roll(second, 4, 0)


def place_block(x, codes, block, extra, keep, base, b, sent, half, links):
    rows = block.shape[1] // BS
    for i in range(rows):
        parts = []
        for g in range(sent // 8):
            part, gs = divmod(8 * g, half)
            s, lanes = side_spot(0, half, block.shape[1], gs)
            here = slice(i * BS, (i + 1) * BS)
            over = 8 * g - keep
            if over < 0:
                main = block[8 * g : 8 * g + 8, here]
            else:
                over += base + half * LANES // block.shape[1]
                main = extra[over : over + 8, here]
            parts.append((main, extra[base + s : base + s + 8, lanes], part * 2 * rows * RIM))
        at = b * rows + i
        place_row(x, i, at, parts, rows)
        for k in range(links):
            s = LA + k
            codes[k, 8 * b + i : 8 * b + i + 1, :] = x[s : s + 1, at * WIDE : (at + 1) * WIDE]


def slot_of(rows):
    return lambda i: i + (i // rows) * (8 - rows)


def split_rows(high, low, j, ref, first, rows, sent):
    for i in range(rows):
        value = ref[0:sent, (first + i) * WIDE : (first + i) * WIDE + LANES]
        top = value.astype(BF16)
        here = slice(i * BS, (i + 1) * BS)
        high[j * sent : (j + 1) * sent, here] = top
        low[j * sent : (j + 1) * sent, here] = (value - top.astype(F32)).astype(BF16)


def inner_body(rows, links, sent, levels, above, own, below, more_above, more, more_below, x0, x1, x2, coef, high, low, codes):
    groups = sent // 8
    slot = slot_of(rows)
    lo, hi, mid = rows, 4 * rows, 2 * rows

    @pl.when(lax.axis_index("grp") == 0)
    def _():
        codes[...] = jnp.zeros(codes.shape, F32)
        for b, block, extra in ((1, above, more_above), (2, own, more), (3, below, more_below)):
            place_block(
                x0, codes, block, extra, block.shape[0], 0, b, sent, levels // 2, links
            )
        tap_counts(codes, coef, 8, 0, links, 8, 24)
        stencil(x0, x1, coef, groups, lo + HALO, hi - lo - 2 * HALO, 3, 1, slot)
        stencil(x1, x2, coef, groups, lo + 2 * HALO, hi - lo - 4 * HALO, 3, 1, slot)
        used = (STEPS + 1) * sent
        high[used:, :] = jnp.zeros((high.shape[0] - used, high.shape[1]), BF16)
        low[used:, :] = jnp.zeros((high.shape[0] - used, high.shape[1]), BF16)
        for j, ref in enumerate((x0, x1, x2)):
            split_rows(high, low, j, ref, mid, rows, sent)


def state_body(rows, links, sent, keep, far_up, far_dn, x0_, x1_, x2_, coef_, high_, low_, powers, xin,
               near_sum, own_mix, own_flux, lift, table, out, x0, x1, x2, coef, high, low, x3, codes):
    levels, cells = out.shape
    groups = sent // 8
    total = 5 * rows
    ocean = lax.axis_index("grp") == 1
    slot = slot_of(rows)

    @pl.when(ocean)
    def _():
        start = xin[...]
        now = (
            dot(own_mix[:, 0:levels], start)
            + dot(own_mix[:, levels:], near_sum[...])
            + dot(lift[0:levels, :], own_flux[...])
        )
        wet = table[2 * links : 2 * links + 1, :]
        out[...] = start + wet * (now - start)

    @pl.when(jnp.logical_not(ocean))
    def _():
        codes[...] = jnp.zeros(codes.shape, F32)
        for b, block in ((0, far_up), (4, far_dn)):
            place_block(x0, codes, block, block, keep, keep, b, sent, levels // 2, links)
            tap_counts(codes, coef, 8, 0, links, 8 * b, 8)

        def apply(src, dst, j, done=None):
            lo, hi = HALO * j, total - HALO * j
            if done is None:
                stencil(src, dst, coef, groups, lo, hi - lo, 3, 1, slot)
                return
            stencil(src, dst, coef, groups, lo, done[0] - lo, 3, 1, slot)
            stencil(src, dst, coef, groups, done[1], hi - done[1], 3, 1, slot)

        mid = 2 * rows
        apply(x0, x1, 1, (rows + HALO, 4 * rows - HALO))
        apply(x1, x2, 2, (rows + 2 * HALO, 4 * rows - 2 * HALO))
        apply(x2, x3, 3)
        split_rows(high, low, 3, x3, mid, rows, sent)
        apply(x3, x0, 4)
        split_rows(high, low, 4, x0, mid, rows, sent)
        top = powers[...]

        def mm(a, b):
            return jnp.dot(a, b, preferred_element_type=F32)

        one = mm(top, high[...])
        two = mm(top[0:sent, :], low[...])
        out[0:sent, :] = one[0:sent, :] + one[sent : 2 * sent, :] + two
        if sent < levels:
            out[sent:levels, :] = jnp.zeros((levels - sent, cells), F32)


def local(
    column_state,
    neighbours,
    mixing,
    diffusivity,
    flux_map,
    force_map,
    return_map,
    sources,
    remap_weights,
    wet,
):
    levels, cells = column_state.shape[1:]
    rows = cells // BS
    links = neighbours.shape[1]
    nf, nr = flux_map.shape[0], return_map.shape[0]
    near = -(-RIM // rows)
    n = 2 * near + 1
    sent = max(up8(LA + links), levels // 2)
    n_reg, n_sub = lax.axis_size("reg"), lax.axis_size("sub")
    axes = ("grp", "reg", "sub")

    def at(g, r, s):
        return (g * n_reg + r % n_reg) * n_sub + s % n_sub

    spots = [(r, s) for r in range(n_reg) for s in range(n_sub)]

    def shift(x, axis, d):
        size = lax.axis_size(axis)
        return lax.ppermute(x, axis, [((i + d) % size, i) for i in range(size)])

    def stack_rows(parts, count):
        out, at = None, 0
        for p in parts:
            here = jnp.pad(p, ((at, up8(count) - at - p.shape[0]), (0, 0)))
            at += p.shape[0]
            out = here if out is None else out + here
        return out

    whole_numbers = stack_rows(
        [neighbours[0], sources, jnp.zeros((links, cells), jnp.int32), wet[None]], 3 * links + 2
    )
    cell_in = whole_numbers.astype(F32) + jnp.pad(
        remap_weights, ((2 * links, up8(3 * links + 2) - 3 * links), (0, 0))
    )
    small = stack_rows([diffusivity, flux_map, force_map.T, return_map], 1 + 2 * nf + nr)
    ext_rows = up8(nf * (STEPS + 1) + links)
    packed = -(-(STEPS + 1) * sent // LANES) * LANES
    message = levels // 4 + 8 * (cells // LANES)
    xin, to_left, to_right, table = call(
        functools.partial(pack_body, links),
        (
            shape(levels, cells),
            shape(message, LANES),
            shape(message, LANES),
            shape(8, cells),
        ),
        column_state[0], cell_in,
        vmem=8 << 20,
    )
    from_right = shift(to_left, "sub", 1)
    from_left = shift(to_right, "sub", -1)
    fields, face0 = call(
        functools.partial(fields_body, nf, nr, links),
        (shape(ext_rows, levels), shape(8, levels)),
        mixing[0], small,
        vmem=8 << 20,
    )
    powers, own_mix, lift = call(
        functools.partial(powers_body, nf, nr, links, sent),
        (
            shape(2 * sent, packed, dtype=BF16),
            shape(levels, 2 * levels),
            shape(levels + 8, 8),
        ),
        mixing[0], small,
        vmem=8 << 20,
    )
    sides = levels // 2 * LANES // cells
    block = sent - (ext_rows - sides)
    up, dn, far, ext, q0, extra = call(
        side_body,
        (
            shape(block, cells),
            shape(block, cells),
            shape(block + ext_rows, cells),
            shape(ext_rows, cells + LANES),
            shape(8, cells),
            shape(ext_rows, cells + LANES),
        ),
        xin, from_right, from_left, fields, face0,
        scratch=[pltpu.VMEM((levels, LANES), F32)],
        vmem=8 << 20,
    )

    swap = [(at(g, r, s), at(1 - g, r, s)) for g in range(2) for r, s in spots]
    hop = lax.ppermute(ext, axes, swap)
    line = lax.broadcasted_iota(jnp.int32, ext.shape, 0)
    relay = jnp.where((line >= nf * STEPS) & (line < nf * (STEPS + 1)), ext, hop)
    relay = jnp.where(lax.axis_index("grp") == 1, relay, extra)
    got, mains = {0: hop}, {}
    for d in sorted(range(-near, near + 1), key=abs):
        key = d % n_reg
        if key in got:
            continue
        close = abs(d) == 1
        ring = [[(at(g, r + d, s), at(g, r, s)) for r, s in spots] for g in (0, 1)]
        both = ring[0] + ring[1]
        got[key] = lax.ppermute(relay, axes, both if close else ring[1])
        block_sent = (up if d < 0 else dn) if close else far
        mains[key] = lax.ppermute(block_sent, axes, both if close else ring[0])
    ext_blocks = [got[d % n_reg] for d in range(-near, near + 1)]
    above, below = mains[-1 % n_reg], mains[1 % n_reg]

    tables = [table] + [None] * (n_sub - 1)
    tables[1], tables[n_sub - 1] = from_right, from_left
    for d in range(2, n_sub - 1):
        tables[d] = shift(table, "sub", d)
    span = n_sub * cells
    high, low, whole = call(
        functools.partial(onto_body, links, cells, n_sub),
        (shape(cells, span, dtype=BF16), shape(cells, span, dtype=BF16), shape(8, span)),
        *tables,
        vmem=24 << 20,
    )

    ext_o = up8(rows + 2 * HALO)
    near_sum = call(
        functools.partial(ocean_body, rows, links),
        shape(levels, cells),
        xin, cell_in, above, below, up,
        scratch=[
            pltpu.VMEM((levels, (rows + 2 * HALO) * WIDE), F32),
            pltpu.VMEM((levels, (rows + 2 * HALO) * WIDE), F32),
            pltpu.VMEM((links, ext_o, WIDE), F32),
            pltpu.VMEM((TAPS * TAPS, ext_o, WIDE), F32),
        ],
        vmem=16 << 20,
    )

    total = rows * n
    ext_n = up8(total)
    fq = call(
        functools.partial(flux_body, rows, near, nf, links),
        shape(8, cells),
        *ext_blocks, ext, q0, cell_in,
        scratch=[
            pltpu.VMEM((nf * STEPS, total * WIDE), F32),
            pltpu.VMEM((nf * STEPS, total * WIDE), F32),
            pltpu.VMEM((links, ext_n, WIDE), F32),
            pltpu.VMEM((TAPS * TAPS, ext_n, WIDE), F32),
            pltpu.VMEM((8, (rows + 2 * HALO) * WIDE), F32),
            pltpu.VMEM((8, (rows + 2 * HALO) * WIDE), F32),
            pltpu.VMEM((links, ext_o, WIDE), F32),
            pltpu.VMEM((TAPS * TAPS, ext_o, WIDE), F32),
        ],
        vmem=8 << 20,
    )
    blocks = [fq] + [shift(fq, "sub", d) for d in range(1, n_sub)]
    own_flux, coupled = call(
        functools.partial(couple_body, links, nf, nr, n_sub),
        (shape(8, cells), shape(8, cells)),
        *blocks, whole, high, low, lift,
        scratch=[
            pltpu.VMEM((8, span), F32),
            pltpu.VMEM((8, span), F32),
            pltpu.VMEM((8, span // 2), F32),
        ],
        vmem=24 << 20,
    )
    back = lax.ppermute(coupled, axes, [(at(1, r, s), at(0, r, s)) for r, s in spots])

    spread = shape(sent, total * WIDE)
    taps = shape(TAPS * TAPS, 8 * n, WIDE)
    basis = shape(packed, cells, dtype=BF16)
    early = call(
        functools.partial(inner_body, rows, links, sent, levels),
        (spread, spread, spread, taps, basis, basis),
        above, up, below, got[-1 % n_reg], extra, got[1 % n_reg],
        scratch=[pltpu.VMEM((links, 8 * n, WIDE), F32)],
        vmem=20 << 20,
    )
    new_state = call(
        functools.partial(state_body, rows, links, sent, block),
        (shape(levels, cells), spread, spread, spread, taps, basis, basis),
        mains[-2 % n_reg], mains[2 % n_reg], *early, powers, xin, near_sum, own_mix, own_flux,
        lift, table,
        scratch=[
            pltpu.VMEM((sent, total * WIDE), F32),
            pltpu.VMEM((links, 8 * n, WIDE), F32),
        ],
        alias={2 + k: 1 + k for k in range(6)},
        vmem=24 << 20,
    )[0]
    ocean_side = lax.axis_index("grp") == 1
    surface = jnp.where(ocean_side, coupled[:nr], back[:nr])
    return (new_state[None], surface)


def solution(mesh):
    in_specs = (
        P("grp", None, ("reg", "sub")),
        P("grp", None, ("reg", "sub")),
        P("grp", None, None),
        P("grp", None),
        P(),
        P(),
        P(),
        P(None, ("reg", "sub")),
        P(None, ("reg", "sub")),
        P(("reg", "sub")),
    )
    out_specs = (P("grp", None, ("reg", "sub")), P(None, ("reg", "sub")))
    return jax.shard_map(local, mesh=mesh, in_specs=in_specs, out_specs=out_specs, check_vma=False)
```

```python
import functools
import jax
import jax.numpy as jnp
from jax import lax
from jax.experimental import pallas as pl
from jax.experimental.pallas import tpu as pltpu
from jax.sharding import PartitionSpec as P

LA = 90
BS = 128
HALO = 2
STEPS = 4
RIM = HALO * STEPS
TAPS = 2 * HALO + 1
HIGH = lax.Precision.HIGHEST
F32 = jnp.float32
BF16 = jnp.bfloat16
LANES = 128
WIDE = 2 * LANES
PACK = LANES // 4


def up8(n):
    return -(-n // 8) * 8


def dot(a, b):
    return jnp.dot(a, b, precision=HIGH, preferred_element_type=F32)


def lane_of(width=LANES, rows=8):
    return lax.broadcasted_iota(jnp.int32, (rows, width), 1)


def roll(x, shift):
    shift = shift % x.shape[1]
    return x if shift == 0 else pltpu.roll(x, shift, 1)


def call(body, outs, *args, scratch=(), vmem=None, flops=100000, alias=None):
    size = sum(a.size * a.dtype.itemsize for a in args)
    return pl.pallas_call(
        body,
        out_shape=outs,
        in_specs=[pl.BlockSpec(memory_space=pltpu.VMEM) for _ in args],
        out_specs=jax.tree.map(lambda _: pl.BlockSpec(memory_space=pltpu.VMEM), outs),
        scratch_shapes=list(scratch),
        input_output_aliases=alias or {},
        compiler_params=pltpu.CompilerParams(vmem_limit_bytes=vmem),
        cost_estimate=pl.CostEstimate(flops=flops, bytes_accessed=size, transcendentals=0),
    )(*args)


def shape(*dims, dtype=F32):
    return jax.ShapeDtypeStruct(dims, dtype)


def pack_body(links, state, cell_in, xin, to_left, to_right, table):
    levels, cells = xin.shape
    rows = cells // BS
    ocean = lax.axis_index("grp") == 1

    @pl.when(jnp.logical_not(ocean))
    def _():
        level = lax.broadcasted_iota(jnp.int32, (levels, cells), 0)
        xin[...] = jnp.where(level < LA, state[...], 0.0)
        xin[LA : LA + links, :] = cell_in[0:links, :]

    @pl.when(ocean)
    def _():
        xin[...] = state[...]

    lane = lane_of()
    quarter = levels // 4
    span = rows * RIM
    for g in range(quarter // 8):
        left = jnp.zeros((8, LANES), F32)
        right = jnp.zeros((8, LANES), F32)
        for q in range(4):
            for i in range(rows):
                at = q * span + i * RIM
                here = (lane >= at) & (lane < at + RIM)
                block = xin[q * quarter + 8 * g : q * quarter + 8 * g + 8, i * BS : (i + 1) * BS]
                left = jnp.where(here, roll(block, at), left)
                right = jnp.where(here, roll(block, at - (BS - RIM)), right)
        to_left[8 * g : 8 * g + 8, :] = left
        to_right[8 * g : 8 * g + 8, :] = right
    table[...] = cell_in[links : links + 8, :]
    for c in range(cells // LANES):
        part = table[:, c * LANES : (c + 1) * LANES]
        to_left[quarter + 8 * c : quarter + 8 * c + 8, :] = part
        to_right[quarter + 8 * c : quarter + 8 * c + 8, :] = part


def level_matrix(mixing):
    levels = mixing.shape[0]
    row = lax.broadcasted_iota(jnp.int32, (levels, levels), 0)
    col = lax.broadcasted_iota(jnp.int32, (levels, levels), 1)
    full = mixing[...] + jnp.where(row == col, 1.0, 0.0)
    return full, jnp.where((row < LA) & (col < LA), full, 0.0)


def fields_body(nf, nr, links, mixing, small, fields, face0):
    levels = mixing.shape[0]
    full, base = level_matrix(mixing)
    r = small[0:1, :]
    ocean = lax.axis_index("grp") == 1
    at = nf * STEPS
    fields[...] = jnp.zeros(fields.shape, F32)

    @pl.when(jnp.logical_not(ocean))
    def _():
        pair = jnp.concatenate([base * (1.0 - float(links) * r), base * r], axis=1)
        lead = jnp.concatenate([small[1 : 1 + nf, :], jnp.zeros((8 - nf, levels), F32)], axis=0)
        have = [lead]
        total = [jnp.zeros((8, levels), F32) for _ in range(STEPS + 1)]
        for n in range(1, STEPS + 1):
            out = dot(jnp.concatenate(have, axis=0) if len(have) > 1 else have[0], pair)
            new = []
            for j in range(n + 1):
                term = jnp.zeros((8, levels), F32)
                if j < n:
                    term = term + out[8 * j : 8 * j + 8, :levels]
                if j > 0:
                    term = term + out[8 * j - 8 : 8 * j, levels:]
                new.append(term)
                total[j] = total[j] + term
            have = new
        for j in range(STEPS + 1):
            to = nf * ((j - 1) % (STEPS + 1))
            fields[to : to + nf, :] = total[j][0:nf, :] * (1.0 / STEPS)
        k = lax.broadcasted_iota(jnp.int32, (links, levels), 0)
        c = lax.broadcasted_iota(jnp.int32, (links, levels), 1)
        fields[at + nf : at + nf + links, :] = jnp.where(c == LA + k, 1.0, 0.0)
        face0[...] = jnp.zeros(face0.shape, F32)

    @pl.when(ocean)
    def _():
        first = 1 + 2 * nf
        lead = jnp.concatenate(
            [small[first : first + nr, :], jnp.zeros((8 - nr, levels), F32)], axis=0
        )
        through = dot(lead, full)
        face0[...] = through * (1.0 - float(links) * r)
        fields[at : at + nr, :] = (through * r)[0:nr, :]


def powers_body(nf, nr, links, sent, mixing, small, powers, own_mix, lift):
    levels = mixing.shape[0]
    full, base = level_matrix(mixing)
    r = small[0:1, :]
    ocean = lax.axis_index("grp") == 1

    @pl.when(jnp.logical_not(ocean))
    def _():
        def squared(mats):
            n = len(mats)
            prod = dot(jnp.concatenate(mats, axis=0), jnp.concatenate(mats, axis=1))
            outs = []
            for j in range(2 * n - 1):
                term = None
                for a in range(n):
                    b = j - a
                    if 0 <= b < n:
                        piece = prod[a * levels : (a + 1) * levels, b * levels : (b + 1) * levels]
                        term = piece if term is None else term + piece
                outs.append(term)
            return outs

        mats = squared(squared([base * (1.0 - float(links) * r), base * r]))
        wide = powers.shape[1]
        whole = jnp.zeros((sent, wide), F32)
        for j in range(STEPS + 1):
            part = jnp.concatenate(
                [mats[j][0:sent, :], jnp.zeros((sent, wide - levels), F32)], axis=1
            )
            whole = whole + roll(part, j * sent)
        top = whole.astype(BF16)
        powers[0:sent, :] = top
        powers[sent : 2 * sent, :] = (whole - top.astype(F32)).astype(BF16)

    @pl.when(ocean)
    def _():
        own_mix[:, 0:levels] = full * (1.0 - float(links) * r)
        own_mix[:, levels : 2 * levels] = full * r
        first = 1 + 2 * nf
        lead = jnp.concatenate(
            [small[first : first + nr, :], jnp.zeros((8 - nr, levels), F32)], axis=0
        )
        top = jnp.concatenate(
            [small[1 + nf : 1 + 2 * nf, :], jnp.zeros((8 - nf, levels), F32)], axis=0
        )
        lifted = lax.dot_general(
            full, top, (((1,), (1,)), ((), ())), precision=HIGH, preferred_element_type=F32
        )
        lift[0:levels, :] = lifted
        lift[levels : levels + 8, :] = dot(lead, lifted)


def side_body(xin, from_right, from_left, fields, face0, up, dn, far, ext, q0, extra, side_levels):
    levels, cells = xin.shape
    rows = cells // BS
    quarter, half = levels // 4, levels // 2
    span = rows * RIM
    lane = lane_of()
    ocean = lax.axis_index("grp") == 1
    sent = up.shape[0]
    edge = HALO * BS
    for g in range(levels // 8):
        q, at = (8 * g) // quarter, (8 * g) % quarter
        a = roll(from_right[at : at + 8, :], -span * q)
        b = roll(from_left[at : at + 8, :], span - span * q)
        side_levels[8 * g : 8 * g + 8, :] = jnp.where(
            lane < span, a, jnp.where(lane < 2 * span, b, 0.0)
        )
    both = jnp.concatenate([fields[...], face0[...]], axis=0)
    full = dot(both, xin[...])
    n = fields.shape[0]
    ext[:, 0:cells] = full[0:n, :]
    q0[...] = full[n : n + 8, :]
    ext[:, cells : cells + LANES] = dot(fields[...], side_levels[...])
    for g in range(half // 8):
        low = side_levels[8 * g : 8 * g + 8, :]
        high = side_levels[half + 8 * g : half + 8 * g + 8, :]
        both = low + roll(high, 2 * span)
        at, lanes = side_spot(0, half, cells, 8 * g)
        extra[at : at + 8, lanes] = both

    n = half * LANES // cells
    more = extra.shape[0] - n
    extra[n:, 0:cells] = xin[sent : sent + more, :]
    extra[:, cells:] = jnp.zeros((n + more, LANES), F32)

    @pl.when(jnp.logical_not(ocean))
    def _():
        up[...] = xin[0:sent, :]
        dn[...] = xin[0:sent, :]
        far[0:sent, :] = xin[0:sent, :]
        far[sent:, :] = extra[:, 0:cells]

    @pl.when(ocean)
    def _():
        for part in range(2):
            rows_of = slice(part * half, (part + 1) * half)
            lanes_of = slice(part * edge, (part + 1) * edge)
            up[0:half, lanes_of] = xin[rows_of, cells - edge : cells]
            dn[0:half, lanes_of] = xin[rows_of, 0:edge]
        for ref in (up, dn):
            ref[half : half + n, :] = extra[0:n, 0:cells]
            ref[half + n :, :] = jnp.zeros((sent - half - n, cells), F32)


def side_spot(sent, half, cells, gs):
    rows = half * LANES // cells
    c, at = divmod(gs, rows)
    return sent + at, slice(c * LANES, (c + 1) * LANES)


def side_lanes(block, at_right, at_left):
    lane = lane_of()
    a = roll(block, -at_right)
    b = roll(block, LANES - RIM - at_left)
    return jnp.where(lane < RIM, a, jnp.where(lane >= LANES - RIM, b, 0.0))


def place_row(x_ref, i, at, blocks, rows):
    span = rows * RIM
    for g, (main, side, shift) in enumerate(blocks):
        x_ref[8 * g : 8 * g + 8, at * WIDE : at * WIDE + LANES] = main
        x_ref[8 * g : 8 * g + 8, at * WIDE + LANES : (at + 1) * WIDE] = side_lanes(
            side, shift + i * RIM, shift + span + i * RIM
        )


def tap_counts(codes, coef, rows, first_row, links, at=0, count=None, packed=False):
    count, wide = count or codes.shape[1], codes.shape[2]
    row = (lax.broadcasted_iota(jnp.int32, (count, wide), 0) + first_row) % rows
    pcol = lax.broadcasted_iota(jnp.int32, (count, wide), 1) % LANES
    width = BS + 2 * HALO
    kinds = []
    for k in range(links):
        n = codes[k, at : at + count, :].astype(jnp.int32)
        line = ((n.astype(F32) + 0.5) * (1.0 / width)).astype(jnp.int32)
        kinds.append((line - row) * 16 + (n - line * width - pcol))
    for dr in range(TAPS):
        for dc in range(TAPS):
            hits = jnp.zeros((count, wide), F32)
            for k in range(links):
                hits = hits + jnp.where(kinds[k] == dr * 16 + dc, 1.0, 0.0)
            coef[dr * TAPS + dc, at : at + count, :] = roll(hits, dc - HALO)
    if packed:
        lane = lane_of(LANES, 8)
        halo = (lane < RIM) | (lane >= LANES - RIM)

        def pack(o, _):
            for p in range(TAPS):
                for a in range(at, at + count, 8):
                    side = jnp.where(halo, coef[o * TAPS + p, a : a + 8, LANES:], 0.0)
                    moved = [roll(side, PACK * q) for q in range(1, 4)]
                    coef[o * TAPS + p, a : a + 8, LANES:] = (side + moved[0]) + (moved[1] + moved[2])
            return 0

        lax.fori_loop(0, TAPS, pack, 0)


def same(i):
    return i


def stencil(src, dst, coef, groups, first, count, batch, step=1, slot=same):
    def row(i):
        off = [pl.multiple_of((i + dr - HALO) * WIDE, WIDE) for dr in range(TAPS)]
        here = pl.multiple_of(i * WIDE, WIDE)
        for g0 in range(0, groups, batch):
            gs = range(g0, min(g0 + batch, groups))
            acc = {}
            for dr in range(TAPS):
                v = {g: src[8 * g : 8 * g + 8, pl.ds(off[dr], WIDE)] for g in gs}
                for dc in range(TAPS):
                    c = coef[dr * TAPS + dc, pl.ds(slot(i), 1), :]
                    for g in gs:
                        t = c * v[g]
                        acc[g, dc] = t if dr == 0 else acc[g, dc] + t
            for g in gs:
                total = acc[g, HALO]
                for dc in range(TAPS):
                    if dc != HALO:
                        total = total + roll(acc[g, dc], HALO - dc)
                dst[8 * g : 8 * g + 8, pl.ds(here, WIDE)] = total

    def one(o, _):
        for p in range(step):
            row(first + o * step + p)
        return 0

    lax.fori_loop(0, count // step, one, 0)


def stencil_packed(src, dst, coef, groups, first, count, slot):
    lane = lane_of()
    edge = (lane < HALO) | (lane >= LANES - HALO)

    def row(i):
        off = [pl.multiple_of((i + dr - HALO) * WIDE, WIDE) for dr in range(TAPS)]
        here = pl.multiple_of(i * WIDE, WIDE)
        for quad in range(groups // 4):
            acc = {}
            side = slice(8 * quad, 8 * quad + 8)
            mains = [slice(8 * g, 8 * g + 8) for g in range(4 * quad, 4 * quad + 4)]
            for dr in range(TAPS):
                v = [src[m, pl.ds(off[dr], LANES)] for m in mains]
                v.append(src[side, pl.ds(off[dr] + LANES, LANES)])
                for dc in range(TAPS):
                    c = coef[dr * TAPS + dc, pl.ds(slot(i), 1), :]
                    for q in range(5):
                        t = (c[:, 0:LANES] if q < 4 else c[:, LANES:]) * v[q]
                        acc[q, dc] = t if dr == 0 else acc[q, dc] + t
            total = [acc[q, HALO] for q in range(5)]
            crossed = [None] * 5
            for dc in range(TAPS):
                d = dc - HALO
                if d == 0:
                    continue
                for q in range(5):
                    size = LANES if q < 4 else PACK
                    place = lane if q < 4 else lane % PACK
                    over = place >= size - d if d > 0 else place < -d
                    t = roll(acc[q, dc], -d)
                    total[q] = total[q] + jnp.where(over, 0.0, t)
                    t = jnp.where(over, t, 0.0)
                    crossed[q] = t if crossed[q] is None else crossed[q] + t
            for q in range(4):
                into = roll(crossed[4], -PACK * q)
                dst[mains[q], pl.ds(here, LANES)] = total[q] + jnp.where(edge, into, 0.0)
                total[4] = total[4] + roll(crossed[q], PACK * q)
            dst[side, pl.ds(here + LANES, LANES)] = total[4]

    def two(o, _):
        row(first + 2 * o)
        row(first + 2 * o + 1)
        return 0

    lax.fori_loop(0, count // 2, two, 0)


def chain(xa, xb, coef, groups, rows, near, batch, take, step=1):
    total = rows * (2 * near + 1)
    refs = (xa, xb)
    lo = near * rows
    take(0, xa, lo)
    for j in range(1, STEPS + 1):
        src, dst = refs[(j - 1) % 2], refs[j % 2]
        first = lo - RIM + HALO * j
        stencil(src, dst, coef, groups, first, total - 2 * first, batch, step)
        take(j, dst, lo)


def ext_row(block, g, i, rows):
    cells = rows * BS
    main = block[8 * g : 8 * g + 8, i * BS : (i + 1) * BS]
    side = side_lanes(block[8 * g : 8 * g + 8, cells : cells + LANES], i * RIM, (rows + i) * RIM)
    return main, side


def flux_body(rows, near, nf, links, *refs):
    n = 2 * near + 1
    blocks, (mine, q0, cell_in, out, xa, xb, codes, coef, ua, ub, own_codes, own_coef) = (
        refs[:n], refs[n:],
    )
    cells = rows * BS
    groups = nf * STEPS // 8

    @pl.when(lax.axis_index("grp") == 1)
    def _():
        codes[...] = jnp.zeros(codes.shape, F32)
        own_codes[...] = jnp.zeros(own_codes.shape, F32)
        for d in range(n):
            for i in range(rows):
                at = d * rows + i
                for g in range(groups):
                    main, side = ext_row(blocks[d], g, i, rows)
                    xa[8 * g : 8 * g + 8, at * WIDE : at * WIDE + LANES] = main
                    xa[8 * g : 8 * g + 8, at * WIDE + LANES : (at + 1) * WIDE] = side
                main, side = ext_row(blocks[d], groups, i, rows)
                for k in range(links):
                    codes[k, at : at + 1, 0:LANES] = main[nf + k : nf + k + 1, :]
                    codes[k, at : at + 1, LANES:WIDE] = side[nf + k : nf + k + 1, :]
                to = at - near * rows + HALO
                if 0 <= to < rows + 2 * HALO:
                    if d == near:
                        main, side = ext_row(mine, groups, i, rows)
                        for k in range(links):
                            own_codes[k, to : to + 1, 0:LANES] = cell_in[
                                k : k + 1, i * BS : (i + 1) * BS
                            ]
                    ua[:, to * WIDE : to * WIDE + LANES] = main
                    ua[:, to * WIDE + LANES : (to + 1) * WIDE] = side
        tap_counts(own_codes, own_coef, rows, rows - HALO, links)
        stencil(ua, ub, own_coef, 1, HALO, rows, 1, rows)
        tap_counts(codes, coef, rows, 0, links)
        own = blocks[near]
        out[0:nf, :] = own[nf * STEPS : nf * (STEPS + 1), 0:cells]
        for i in range(rows):
            here = slice(i * BS, (i + 1) * BS)
            face = q0[:, here] + ub[:, (HALO + i) * WIDE : (HALO + i) * WIDE + LANES]
            out[nf:8, here] = face[0 : 8 - nf, :]

        def take(j, ref, lo):
            if j == 0:
                return
            at = nf * (j - 1)
            for i in range(rows):
                here = slice(i * BS, (i + 1) * BS)
                out[0:nf, here] = (
                    out[0:nf, here] + ref[at : at + nf, (lo + i) * WIDE : (lo + i) * WIDE + LANES]
                )

        chain(xa, xb, coef, groups, rows, near, groups, take, 4)


def ocean_body(rows, links, xin, cell_in, above, below, own, near, x, y, codes, coef):
    levels, cells = xin.shape
    half, edge = levels // 2, HALO * BS
    groups = levels // 8

    @pl.when(lax.axis_index("grp") == 1)
    def _():
        for at in range(rows + 2 * HALO):
            if at < HALO:
                i, side = rows - HALO + at, above
            elif at < HALO + rows:
                i, side = at - HALO, own
            else:
                i, side = at - HALO - rows, below
            parts = []
            for g in range(groups):
                part, gs = divmod(8 * g, half)
                if at < HALO:
                    main = above[gs : gs + 8, part * edge + at * BS : part * edge + (at + 1) * BS]
                elif at < HALO + rows:
                    main = xin[8 * g : 8 * g + 8, i * BS : (i + 1) * BS]
                else:
                    main = below[gs : gs + 8, part * edge + i * BS : part * edge + (i + 1) * BS]
                s, lanes = side_spot(half, half, cells, gs)
                parts.append((main, side[s : s + 8, lanes], part * 2 * rows * RIM))
            place_row(x, i, at, parts, rows)
        codes[...] = jnp.zeros(codes.shape, F32)
        for k in range(links):
            for i in range(rows):
                codes[k, HALO + i : HALO + i + 1, 0:LANES] = cell_in[
                    k : k + 1, i * BS : (i + 1) * BS
                ]
        tap_counts(codes, coef, rows, rows - HALO, links)
        stencil(x, y, coef, groups, HALO, rows, 3)
        for i in range(rows):
            near[:, i * BS : (i + 1) * BS] = y[:, (HALO + i) * WIDE : (HALO + i) * WIDE + LANES]


def onto_body(links, cells, count, *refs):
    tables, (high, low, whole) = refs[:count], refs[count:]
    me = lax.axis_index("sub")
    for d in range(count):
        at = pl.multiple_of(((me + d) % count) * cells, cells)
        if tables[d].shape[1] == cells:
            whole[:, pl.ds(at, cells)] = tables[d][...]
        else:
            first = tables[d].shape[0] - 8 * (cells // LANES)
            for c in range(cells // LANES):
                whole[:, pl.ds(pl.multiple_of(at + c * LANES, LANES), LANES)] = tables[d][
                    first + 8 * c : first + 8 * c + 8, :
                ]

    @pl.when(lax.axis_index("grp") == 1)
    def _():
        def chunk(c, _):
            at = pl.multiple_of(c * LANES, LANES)
            src = whole[0:links, pl.ds(at, LANES)].astype(jnp.int32) - me * cells
            w = whole[links : 2 * links, pl.ds(at, LANES)]
            for t in range(0, cells, 16):
                target = lax.broadcasted_iota(jnp.int32, (16, LANES), 0) + t
                value = jnp.zeros((16, LANES), F32)
                for k in range(links):
                    value = value + jnp.where(src[k : k + 1, :] == target, w[k : k + 1, :], 0.0)
                top = value.astype(BF16)
                high[t : t + 16, pl.ds(at, LANES)] = top
                low[t : t + 16, pl.ds(at, LANES)] = (value - top.astype(F32)).astype(BF16)
            return 0

        lax.fori_loop(0, count * cells // LANES, chunk, 0)


def stacked(x, y):
    sub = lax.broadcasted_iota(jnp.int32, x.shape, 0)
    return jnp.where(sub < 4, x, pltpu.roll(y, 4, 0))


def couple_body(links, nf, nr, count, *refs):
    blocks, (whole, high, low, lift, own_flux, out, slab, pair, surface) = (
        refs[:count], refs[count:],
    )
    cells = blocks[0].shape[1]
    levels = lift.shape[0] - 8
    me = lax.axis_index("sub")

    @pl.when(lax.axis_index("grp") == 1)
    def _():
        for d in range(count):
            at = pl.multiple_of(((me + d) % count) * cells, cells)
            block = blocks[d][...]
            slab[:, pl.ds(at, cells)] = block
            pair[:, pl.ds(at, cells)] = stacked(block, block)
        chunks = count * cells // LANES
        half = chunks // 2
        per = min(chunks, 16)
        mine = cells // LANES
        sub = lax.broadcasted_iota(jnp.int32, (8, LANES), 0)

        def two(a, b):
            return jnp.where(sub < 4, a, b)

        def target(c):
            at0 = pl.multiple_of(c * LANES, LANES)
            at1 = pl.multiple_of((c + half) * LANES, LANES)
            t0, t1 = whole[:, pl.ds(at0, LANES)], whole[:, pl.ds(at1, LANES)]
            src, w = [], []
            for k in range(links):
                src.append(two(t0[k : k + 1, :], t1[k : k + 1, :]).astype(jnp.int32))
                w.append(two(t0[links + k : links + k + 1, :], t1[links + k : links + k + 1, :]))
            lanes = [x & (LANES - 1) for x in src]
            homes = [x // LANES for x in src]

            def source(o, acc):
                acc = list(acc)
                for p in range(per):
                    b = o * per + p
                    v = pair[:, pl.ds(pl.multiple_of(b * LANES, LANES), LANES)]
                    for k in range(links):
                        got = jnp.take_along_axis(v, lanes[k], axis=1)
                        acc[k] = jnp.where(homes[k] == b, got, acc[k])
                return tuple(acc)

            zero = tuple(jnp.zeros((8, LANES), F32) for _ in range(links))
            got = source(0, zero) if chunks == per else lax.fori_loop(0, chunks // per, source, zero)
            flux = w[0] * got[0]
            for k in range(1, links):
                flux = flux + w[k] * got[k]
            s0, s1 = slab[:, pl.ds(at0, LANES)], slab[:, pl.ds(at1, LANES)]
            face = stacked(pltpu.roll(s0, 8 - nf, 0), pltpu.roll(s1, 8 - nf, 0))
            col = lift[levels : levels + 8, :]
            col = stacked(col, col)
            for f in range(nf):
                face = face + col[:, f : f + 1] * two(flux[f : f + 1, :], flux[4 + f : 5 + f, :])
            n = 2 * links
            face = jnp.where(
                sub % 4 < nr, face * two(t0[n : n + 1, :], t1[n : n + 1, :]), 0.0
            )
            surface[:, pl.ds(at0, LANES)] = face
            for part, lift_rows in ((0, flux), (1, pltpu.roll(flux, 4, 0))):
                here = c + part * half - me * mine

                @pl.when((here >= 0) & (here < mine))
                def _():
                    own_flux[:, pl.ds(pl.multiple_of(here * LANES, LANES), LANES)] = jnp.where(
                        sub < nf, lift_rows, 0.0
                    )

        def some(o, _):
            for p in range(2):
                target(o * 2 + p)
            return 0

        lax.fori_loop(0, half // 2, some, 0)
        face = surface[...]
        top = face.astype(BF16)
        rest = (face - top.astype(F32)).astype(BF16)
        both = jnp.concatenate([top, rest], axis=0)

        def nt(a, b):
            return lax.dot_general(a, b, (((1,), (1,)), ((), ())), preferred_element_type=F32)

        cut = half * LANES
        one = nt(both, high[:, 0:cut])
        two_ = nt(top, low[:, 0:cut])
        three = nt(both, high[:, cut : 2 * cut])
        four = nt(top, low[:, cut : 2 * cut])
        first = one[0:8, :] + one[8:16, :] + two_
        second = three[0:8, :] + three[8:16, :] + four
        out[...] = first + pltpu.roll(second, 4, 0)


def place_block(x, codes, block, extra, keep, base, b, sent, half, links):
    rows = block.shape[1] // BS
    span = rows * RIM
    first = base + half * LANES // block.shape[1] - keep
    lane = lane_of()
    for i in range(rows):
        at = b * rows + i
        here = slice(i * BS, (i + 1) * BS)
        total = None
        for g in range(sent // 8):
            part, gs = divmod(8 * g, half)
            s, lanes = side_spot(base, half, block.shape[1], gs)
            if 8 * g < keep:
                main = block[8 * g : 8 * g + 8, here]
            else:
                main = extra[first + 8 * g : first + 8 * g + 8, here]
            shift = 2 * span * part + i * RIM
            x[8 * g : 8 * g + 8, at * WIDE : at * WIDE + LANES] = main
            if g == LA // 8:
                side = side_lanes(extra[s : s + 8, lanes], shift, shift + span)
                for k in range(links):
                    n = LA % 8 + k
                    codes[k, 8 * b + i : 8 * b + i + 1, 0:LANES] = main[n : n + 1, :]
                    codes[k, 8 * b + i : 8 * b + i + 1, LANES:WIDE] = side[n : n + 1, :]
            if g % 4 == 0:
                total = jnp.zeros((8, LANES), F32)
            to = PACK * (g % 4)
            place = (lane - to) & (LANES - 1)
            source = extra[s : s + 8, lanes]
            total = jnp.where(place < RIM, roll(source, to - shift), total)
            total = jnp.where(place >= LANES - RIM, roll(source, to - RIM - shift - span), total)
            if g % 4 == 3:
                x[8 * (g // 4) : 8 * (g // 4) + 8, at * WIDE + LANES : (at + 1) * WIDE] = total


def slot_of(rows):
    return lambda i: i + (i // rows) * (8 - rows)


def split_rows(high, low, j, ref, first, rows, sent):
    for i in range(rows):
        value = ref[0:sent, (first + i) * WIDE : (first + i) * WIDE + LANES]
        top = value.astype(BF16)
        here = slice(i * BS, (i + 1) * BS)
        high[j * sent : (j + 1) * sent, here] = top
        low[j * sent : (j + 1) * sent, here] = (value - top.astype(F32)).astype(BF16)


def inner_body(rows, links, sent, levels, above, own, below, more_above, more, more_below, x0, x1, x2, coef, high, low, codes):
    groups = sent // 8
    slot = slot_of(rows)
    lo, hi, mid = rows, 4 * rows, 2 * rows

    @pl.when(lax.axis_index("grp") == 0)
    def _():
        codes[...] = jnp.zeros(codes.shape, F32)
        for b, block, extra in ((1, above, more_above), (2, own, more), (3, below, more_below)):
            place_block(
                x0, codes, block, extra, block.shape[0], 0, b, sent, levels // 2, links
            )
        tap_counts(codes, coef, 8, 0, links, 8, 24, True)
        stencil_packed(x0, x1, coef, groups, lo + HALO, hi - lo - 2 * HALO, slot)
        stencil_packed(x1, x2, coef, groups, lo + 2 * HALO, hi - lo - 4 * HALO, slot)
        used = (STEPS + 1) * sent
        high[used:, :] = jnp.zeros((high.shape[0] - used, high.shape[1]), BF16)
        low[used:, :] = jnp.zeros((high.shape[0] - used, high.shape[1]), BF16)
        for j, ref in enumerate((x0, x1, x2)):
            split_rows(high, low, j, ref, mid, rows, sent)


def state_body(rows, links, sent, keep, far_up, far_dn, x0_, x1_, x2_, coef_, high_, low_, powers, xin,
               near_sum, own_mix, own_flux, lift, table, out, x0, x1, x2, coef, high, low, x3, codes):
    levels, cells = out.shape
    groups = sent // 8
    total = 5 * rows
    ocean = lax.axis_index("grp") == 1
    slot = slot_of(rows)

    @pl.when(ocean)
    def _():
        start = xin[...]
        now = (
            dot(own_mix[:, 0:levels], start)
            + dot(own_mix[:, levels:], near_sum[...])
            + dot(lift[0:levels, :], own_flux[...])
        )
        wet = table[2 * links : 2 * links + 1, :]
        out[...] = start + wet * (now - start)

    @pl.when(jnp.logical_not(ocean))
    def _():
        codes[...] = jnp.zeros(codes.shape, F32)
        for b, block in ((0, far_up), (4, far_dn)):
            place_block(x0, codes, block, block, keep, keep, b, sent, levels // 2, links)
            tap_counts(codes, coef, 8, 0, links, 8 * b, 8, True)

        def apply(src, dst, j, done=None):
            lo, hi = HALO * j, total - HALO * j
            if done is None:
                stencil_packed(src, dst, coef, groups, lo, hi - lo, slot)
                return
            stencil_packed(src, dst, coef, groups, lo, done[0] - lo, slot)
            stencil_packed(src, dst, coef, groups, done[1], hi - done[1], slot)

        mid = 2 * rows
        apply(x0, x1, 1, (rows + HALO, 4 * rows - HALO))
        apply(x1, x2, 2, (rows + 2 * HALO, 4 * rows - 2 * HALO))
        apply(x2, x3, 3)
        split_rows(high, low, 3, x3, mid, rows, sent)
        apply(x3, x0, 4)
        split_rows(high, low, 4, x0, mid, rows, sent)
        top = powers[...]

        def mm(a, b):
            return jnp.dot(a, b, preferred_element_type=F32)

        one = mm(top, high[...])
        two = mm(top[0:sent, :], low[...])
        out[0:sent, :] = one[0:sent, :] + one[sent : 2 * sent, :] + two
        if sent < levels:
            out[sent:levels, :] = jnp.zeros((levels - sent, cells), F32)


def local(
    column_state,
    neighbours,
    mixing,
    diffusivity,
    flux_map,
    force_map,
    return_map,
    sources,
    remap_weights,
    wet,
):
    levels, cells = column_state.shape[1:]
    rows = cells // BS
    links = neighbours.shape[1]
    nf, nr = flux_map.shape[0], return_map.shape[0]
    near = -(-RIM // rows)
    n = 2 * near + 1
    sent = max(up8(LA + links), levels // 2)
    n_reg, n_sub = lax.axis_size("reg"), lax.axis_size("sub")
    axes = ("grp", "reg", "sub")

    def at(g, r, s):
        return (g * n_reg + r % n_reg) * n_sub + s % n_sub

    spots = [(r, s) for r in range(n_reg) for s in range(n_sub)]

    def shift(x, axis, d):
        size = lax.axis_size(axis)
        return lax.ppermute(x, axis, [((i + d) % size, i) for i in range(size)])

    def stack_rows(parts, count):
        out, at = None, 0
        for p in parts:
            here = jnp.pad(p, ((at, up8(count) - at - p.shape[0]), (0, 0)))
            at += p.shape[0]
            out = here if out is None else out + here
        return out

    whole_numbers = stack_rows(
        [neighbours[0], sources, jnp.zeros((links, cells), jnp.int32), wet[None]], 3 * links + 2
    )
    cell_in = whole_numbers.astype(F32) + jnp.pad(
        remap_weights, ((2 * links, up8(3 * links + 2) - 3 * links), (0, 0))
    )
    small = stack_rows([diffusivity, flux_map, force_map.T, return_map], 1 + 2 * nf + nr)
    ext_rows = up8(nf * (STEPS + 1) + links)
    packed = -(-(STEPS + 1) * sent // LANES) * LANES
    message = levels // 4 + 8 * (cells // LANES)
    xin, to_left, to_right, table = call(
        functools.partial(pack_body, links),
        (
            shape(levels, cells),
            shape(message, LANES),
            shape(message, LANES),
            shape(8, cells),
        ),
        column_state[0], cell_in,
        vmem=8 << 20,
    )
    from_right = shift(to_left, "sub", 1)
    from_left = shift(to_right, "sub", -1)
    fields, face0 = call(
        functools.partial(fields_body, nf, nr, links),
        (shape(ext_rows, levels), shape(8, levels)),
        mixing[0], small,
        vmem=8 << 20,
    )
    powers, own_mix, lift = call(
        functools.partial(powers_body, nf, nr, links, sent),
        (
            shape(2 * sent, packed, dtype=BF16),
            shape(levels, 2 * levels),
            shape(levels + 8, 8),
        ),
        mixing[0], small,
        vmem=8 << 20,
    )
    sides = levels // 2 * LANES // cells
    block = sent - (ext_rows - sides)
    up, dn, far, ext, q0, extra = call(
        side_body,
        (
            shape(block, cells),
            shape(block, cells),
            shape(block + ext_rows, cells),
            shape(ext_rows, cells + LANES),
            shape(8, cells),
            shape(ext_rows, cells + LANES),
        ),
        xin, from_right, from_left, fields, face0,
        scratch=[pltpu.VMEM((levels, LANES), F32)],
        vmem=8 << 20,
    )

    swap = [(at(g, r, s), at(1 - g, r, s)) for g in range(2) for r, s in spots]
    hop = lax.ppermute(ext, axes, swap)
    line = lax.broadcasted_iota(jnp.int32, ext.shape, 0)
    relay = jnp.where((line >= nf * STEPS) & (line < nf * (STEPS + 1)), ext, hop)
    relay = jnp.where(lax.axis_index("grp") == 1, relay, extra)
    got, mains = {0: hop}, {}
    for d in sorted(range(-near, near + 1), key=abs):
        key = d % n_reg
        if key in got:
            continue
        close = abs(d) == 1
        ring = [[(at(g, r + d, s), at(g, r, s)) for r, s in spots] for g in (0, 1)]
        both = ring[0] + ring[1]
        got[key] = lax.ppermute(relay, axes, both if close else ring[1])
        block_sent = (up if d < 0 else dn) if close else far
        mains[key] = lax.ppermute(block_sent, axes, both if close else ring[0])
    ext_blocks = [got[d % n_reg] for d in range(-near, near + 1)]
    above, below = mains[-1 % n_reg], mains[1 % n_reg]

    tables = [table] + [None] * (n_sub - 1)
    tables[1], tables[n_sub - 1] = from_right, from_left
    for d in range(2, n_sub - 1):
        tables[d] = shift(table, "sub", d)
    span = n_sub * cells
    high, low, whole = call(
        functools.partial(onto_body, links, cells, n_sub),
        (shape(cells, span, dtype=BF16), shape(cells, span, dtype=BF16), shape(8, span)),
        *tables,
        vmem=24 << 20,
    )

    ext_o = up8(rows + 2 * HALO)
    near_sum = call(
        functools.partial(ocean_body, rows, links),
        shape(levels, cells),
        xin, cell_in, above, below, up,
        scratch=[
            pltpu.VMEM((levels, (rows + 2 * HALO) * WIDE), F32),
            pltpu.VMEM((levels, (rows + 2 * HALO) * WIDE), F32),
            pltpu.VMEM((links, ext_o, WIDE), F32),
            pltpu.VMEM((TAPS * TAPS, ext_o, WIDE), F32),
        ],
        vmem=16 << 20,
    )

    total = rows * n
    ext_n = up8(total)
    fq = call(
        functools.partial(flux_body, rows, near, nf, links),
        shape(8, cells),
        *ext_blocks, ext, q0, cell_in,
        scratch=[
            pltpu.VMEM((nf * STEPS, total * WIDE), F32),
            pltpu.VMEM((nf * STEPS, total * WIDE), F32),
            pltpu.VMEM((links, ext_n, WIDE), F32),
            pltpu.VMEM((TAPS * TAPS, ext_n, WIDE), F32),
            pltpu.VMEM((8, (rows + 2 * HALO) * WIDE), F32),
            pltpu.VMEM((8, (rows + 2 * HALO) * WIDE), F32),
            pltpu.VMEM((links, ext_o, WIDE), F32),
            pltpu.VMEM((TAPS * TAPS, ext_o, WIDE), F32),
        ],
        vmem=8 << 20,
    )
    blocks = [fq] + [shift(fq, "sub", d) for d in range(1, n_sub)]
    own_flux, coupled = call(
        functools.partial(couple_body, links, nf, nr, n_sub),
        (shape(8, cells), shape(8, cells)),
        *blocks, whole, high, low, lift,
        scratch=[
            pltpu.VMEM((8, span), F32),
            pltpu.VMEM((8, span), F32),
            pltpu.VMEM((8, span // 2), F32),
        ],
        vmem=24 << 20,
    )
    back = lax.ppermute(coupled, axes, [(at(1, r, s), at(0, r, s)) for r, s in spots])

    spread = shape(sent, total * WIDE)
    taps = shape(TAPS * TAPS, 8 * n, WIDE)
    basis = shape(packed, cells, dtype=BF16)
    early = call(
        functools.partial(inner_body, rows, links, sent, levels),
        (spread, spread, spread, taps, basis, basis),
        above, up, below, got[-1 % n_reg], extra, got[1 % n_reg],
        scratch=[pltpu.VMEM((links, 8 * n, WIDE), F32)],
        vmem=20 << 20,
    )
    new_state = call(
        functools.partial(state_body, rows, links, sent, block),
        (shape(levels, cells), spread, spread, spread, taps, basis, basis),
        mains[-2 % n_reg], mains[2 % n_reg], *early, powers, xin, near_sum, own_mix, own_flux,
        lift, table,
        scratch=[
            pltpu.VMEM((sent, total * WIDE), F32),
            pltpu.VMEM((links, 8 * n, WIDE), F32),
        ],
        alias={2 + k: 1 + k for k in range(6)},
        vmem=24 << 20,
    )[0]
    ocean_side = lax.axis_index("grp") == 1
    surface = jnp.where(ocean_side, coupled[:nr], back[:nr])
    return (new_state[None], surface)


def solution(mesh):
    in_specs = (
        P("grp", None, ("reg", "sub")),
        P("grp", None, ("reg", "sub")),
        P("grp", None, None),
        P("grp", None),
        P(),
        P(),
        P(),
        P(None, ("reg", "sub")),
        P(None, ("reg", "sub")),
        P(("reg", "sub")),
    )
    out_specs = (P("grp", None, ("reg", "sub")), P(None, ("reg", "sub")))
    return jax.shard_map(local, mesh=mesh, in_specs=in_specs, out_specs=out_specs, check_vma=False)
```
